32 devices in a mesh: row: 4 (over z), col: 8 (over y, x, core).
Axes of the slice: x: 2, y: 2, z: 4, core: 2. Of those that a mesh axis runs over, the one named last changes fastest.
Arguments:
- cell_index: int32 [2, 3, 65536], P(None, None, ('row', 'col')), may hold values from 0 to 255, as said below
- fraction: float32 [2, 3, 65536], P(None, None, ('row', 'col')), may hold values from 0 to 1
- charge: float32 [2, 65536], P(None, ('row', 'col')), may hold values from -4 to 4
- atom_count: int32 [2, 32], P(None, ('row', 'col')), may hold values from 1024 to 2048, as said below
- influence: float32 [256, 256, 256], P('row', 'col'), as said below
Outputs:
- forces: float32 [2, 3, 65536], P(None, None, ('row', 'col'))
The draws below stay inside these ranges and needn't reach their ends.
Inputs may be any that keep to these rules, and one draw needn't show every extreme that they name: `cell_index`: slot a belongs to pencil p = a // 2048; with P = 8, its first cell index lies in [(p // P) * 64, (p // P + 1) * 64) and its second in [(p % P) * 32, (p % P + 1) * 32). `atom_count`: in every frame some pencil has all 2048 slots live. Even: influence[a, b, c] equals influence[(-a) mod 256, (-b) mod 256, (-c) mod 256]; it is 0 at the root and positive elsewhere.
All inputs are finite; a program needn't handle non-finite values.
Results may differ from the reference program's by a relative error of at most 0.0003.
Values sent between devices are 32-bit elements; how exact they have to be, the bound alone decides.
A program may use at most 128 MiB of HBM per device.

```python
import math
import jax
import jax.numpy as jnp

K = 256
ATOM_DEV = 2048
STEPS = 2
XB = 64
YB = 32
PENCILS = 32
ATOMS = 65536


def draw_cell_index(key, part):
    per_row = K // YB
    slot_ids = jnp.arange(ATOMS, dtype=jnp.int32)
    pencil = slot_ids // ATOM_DEV
    first_base = pencil // per_row * XB
    second_base = pencil % per_row * YB
    subkeys = jax.random.split(key, 3)
    first_index = first_base[None, :] + jax.random.randint(subkeys[0], (STEPS, ATOMS), 0, XB)
    second_index = second_base[None, :] + jax.random.randint(subkeys[1], (STEPS, ATOMS), 0, YB)
    third_index = jax.random.randint(subkeys[2], (STEPS, ATOMS), 0, K)
    return jnp.stack([first_index, second_index, third_index], axis=1).astype(jnp.int32)


def draw_atom_count(key, part):
    subkeys = jax.random.split(key, 2)
    counts = jax.random.randint(subkeys[0], (STEPS, PENCILS), ATOM_DEV // 2, ATOM_DEV + 1)
    chosen = jax.random.randint(subkeys[1], (STEPS, 1), 0, PENCILS)
    column = jnp.arange(PENCILS, dtype=jnp.int32)
    return jnp.where(column[None, :] == chosen, ATOM_DEV, counts).astype(jnp.int32)


def draw_influence(key, part):
    wave_index = jnp.arange(K, dtype=jnp.int32)
    roughness = jnp.exp(jax.random.uniform(key, (K, K, K), jnp.float32, math.log(2.0), math.log(40.0)))
    mirror = jnp.roll(jnp.flip(roughness, (0, 1, 2)), 1, axis=(0, 1, 2))
    symmetric = 0.5 * (roughness + mirror)
    root = (wave_index[:, None, None] == 0) & (wave_index[None, :, None] == 0) & (wave_index[None, None, :] == 0)
    return jnp.where(root, 0.0, symmetric).astype(jnp.float32)


def steps_of(key, shape, cuts, smallest, high):
    factor_of, own = 1.0, jax.random.fold_in(key, 6)
    for position, blocks in cuts:
        steps = jnp.exp(jax.random.uniform(jax.random.fold_in(own, position), (blocks,), jnp.float32, smallest / len(cuts), high / len(cuts)))
        factor_of = factor_of * jnp.repeat(steps, shape[position] // blocks).reshape([-1 if axis == position else 1 for axis in range(len(shape))])
    return factor_of


def scatter_about(rng, extent, spread, limit, pieces=(), kind=jnp.bfloat16):
    values = jax.random.normal(rng, extent, jnp.float32) * spread
    if len(pieces) > 0:
        values = steps_of(rng, extent, pieces, -0.22, 0.18) * values
    return jnp.clip(values, min=-limit, max=limit).astype(kind)


def setup_inputs(seed: int = 0) -> dict:
    splits = jax.random.split(jax.random.key(seed), 6)
    return {
        "cell_index": draw_cell_index(jax.random.fold_in(splits[5], 71), 0),
        "fraction": jnp.clip(1.0 * jax.random.uniform(splits[1], (STEPS, 3, ATOMS), jnp.float32) ** steps_of(splits[1], (STEPS, 3, ATOMS), ((2, 32),), -0.2, 0.2), 0.0, 1.0),
        "charge": scatter_about(splits[2], (STEPS, ATOMS), 1.0, 4.0, ((1, 32),), jnp.float32),
        "atom_count": draw_atom_count(jax.random.fold_in(splits[5], 71), 0),
        "influence": draw_influence(jax.random.fold_in(splits[5], 71), 0),
    }


def spline_values(fraction):
    nothing = jnp.zeros_like(fraction)
    levels = [fraction, 1.0 - fraction]
    slopes = levels
    for degree in range(3, 7):
        padded = levels + [nothing]
        following = []
        for offset in range(degree):
            beneath = padded[offset - 1] if offset > 0 else nothing
            following.append(((fraction + offset) * padded[offset] + (degree - fraction - offset) * beneath) / (degree - 1))
        if degree == 6:
            slopes = [padded[offset] - (padded[offset - 1] if offset > 0 else nothing) for offset in range(6)]
        levels = following
    return jnp.stack(levels), jnp.stack(slopes)


def reference(cell_index, fraction, charge, atom_count, influence):
    slot_ids = jnp.arange(ATOMS, dtype=jnp.int32)
    pencil = slot_ids // ATOM_DEV
    green_table = jnp.transpose(influence, (2, 0, 1))
    offsets = jnp.arange(6, dtype=jnp.int32)
    results = []
    for step in range(STEPS):
        living = (slot_ids % ATOM_DEV) < atom_count[step][pencil]
        charges = jnp.where(living, charge[step], 0.0)
        values = []
        slopes = []
        corners = []
        for dimension in range(3):
            weight, gradient = spline_values(fraction[step, dimension])
            values.append(weight)
            slopes.append(gradient)
            corners.append(((cell_index[step, dimension][None, :] - offsets[:, None]) % K).astype(jnp.int32))
        index_inner = corners[1][:, None, :] * K + corners[2][None, :, :]
        weight_inner = values[1][:, None, :] * values[2][None, :, :]
        charge_mesh = jnp.zeros((K * K * K,), jnp.float32)
        for offset in range(6):
            target = corners[0][offset][None, None, :] * (K * K) + index_inner
            amount = charges[None, None, :] * values[0][offset][None, None, :] * weight_inner
            charge_mesh = charge_mesh.at[target.reshape(-1)].add(amount.reshape(-1))
        spectrum = jnp.fft.fftn(charge_mesh.reshape(K, K, K))
        potential = jnp.real(jnp.fft.ifftn(green_table * spectrum)).reshape(-1)
        first_total = jnp.zeros_like(charges)
        second_total = jnp.zeros_like(charges)
        third_total = jnp.zeros_like(charges)
        for offset in range(6):
            target = corners[0][offset][None, None, :] * (K * K) + index_inner
            sampled = potential[target]
            first_total = first_total + slopes[0][offset] * jnp.sum(sampled * weight_inner, axis=(0, 1))
            second_total = second_total + values[0][offset] * jnp.sum(sampled * slopes[1][:, None, :] * values[2][None, :, :], axis=(0, 1))
            third_total = third_total + values[0][offset] * jnp.sum(sampled * values[1][:, None, :] * slopes[2][None, :, :], axis=(0, 1))
        results.append(-charges[None, :] * jnp.stack([first_total, second_total, third_total]))
    return jnp.stack(results)
```

```python
import functools
import math

import jax
import jax.numpy as jnp
from jax import lax
from jax.experimental import pallas as pl
from jax.experimental.pallas import tpu as pltpu
from jax.sharding import PartitionSpec as P

MESH = pl.DeviceIdType.MESH
LANES = 128
CHUNK = 9
HALO = 8
NT = (((1,), (1,)), ((), ()))
NN = (((1,), (0,)), ((), ()))


def dot(left, right, form=NN):
    return lax.dot_general(left, right, form, preferred_element_type=jnp.float32)


def halves_of(value):
    high = value.astype(jnp.bfloat16)
    return high, (value - high.astype(jnp.float32)).astype(jnp.bfloat16)


def spline_rows(fraction):
    nothing = jnp.zeros_like(fraction)
    levels = [fraction, 1.0 - fraction]
    slopes = levels
    for degree in range(3, 7):
        padded = levels + [nothing]
        following = []
        for offset in range(degree):
            beneath = padded[offset - 1] if offset > 0 else nothing
            following.append(
                ((fraction + offset) * padded[offset] + (degree - fraction - offset) * beneath)
                * (1.0 / (degree - 1))
            )
        if degree == 6:
            slopes = [
                padded[offset] - (padded[offset - 1] if offset > 0 else nothing)
                for offset in range(6)
            ]
        levels = following
    return levels, slopes


def dense(distance, lists):
    results = [jnp.zeros(distance.shape, jnp.float32) for _ in lists]
    for offset in range(6):
        hit = distance == offset
        results = [jnp.where(hit, rows[offset], result) for rows, result in zip(lists, results)]
    return results


def row_of(lists, dimension):
    return [entry[dimension : dimension + 1, :] for entry in lists]


def phases(product, length):
    half = length // 2
    moved = product + half
    if length & (length - 1):
        turned = lax.rem(moved, length) - half
    else:
        turned = (moved & (length - 1)) - half
    angle = turned.astype(jnp.float32) * (2.0 * math.pi / length / 4.0)
    square = angle * angle
    sine = angle * (
        1.0
        + square
        * (-1.0 / 6 + square * (1.0 / 120 + square * (-1.0 / 5040 + square * (1.0 / 362880))))
    )
    cosine = 1.0 + square * (
        -0.5
        + square
        * (1.0 / 24 + square * (-1.0 / 720 + square * (1.0 / 40320 - square * (1.0 / 3628800))))
    )
    for _ in range(2):
        sine, cosine = 2.0 * sine * cosine, 1.0 - 2.0 * sine * sine
    return cosine, sine


def wave_rows(cosine, sine, cos_ref, sin_ref, rows):
    even = cos_ref[0] * rows[0]
    odd = sin_ref[0] * rows[0]
    for offset in range(1, 6):
        even += cos_ref[offset] * rows[offset]
        odd += sin_ref[offset] * rows[offset]
    return cosine * even + sine * odd


def sort_kernel(key_row_ref, key_col_ref, payload_ref, sorted_ref, rank_ref):
    atoms = key_row_ref.shape[2]

    @pl.loop(0, atoms // LANES)
    def count(part):
        lanes = pl.ds(pl.multiple_of(part * LANES, LANES), LANES)
        below = key_col_ref[0] < key_row_ref[0, :, lanes]
        rank_ref[0, :, lanes] = jnp.sum(jnp.where(below, 1.0, 0.0), axis=0, keepdims=True)

    value = payload_ref[0]
    first, rest = halves_of(value)
    left = value - first.astype(jnp.float32)
    third = (left - rest.astype(jnp.float32)).astype(jnp.bfloat16)
    pieces = jnp.concatenate([first, rest, third, jnp.zeros_like(first)], axis=0)
    rank = rank_ref[0].astype(jnp.int32)
    width = math.gcd(256, atoms)

    @pl.loop(0, atoms // width)
    def place(part):
        start = pl.multiple_of(part * width, width)
        spots = lax.broadcasted_iota(jnp.int32, (width, atoms), 0) + start
        chosen = jnp.where(rank == spots, 1.0, 0.0).astype(jnp.bfloat16)
        moved = dot(pieces, chosen, NT)
        sorted_ref[0, :, pl.ds(start, width)] = moved[0:8] + moved[8:16] + moved[16:24]


def sort_atoms(key_row, key_col, payload):
    frames, rows, atoms = payload.shape
    whole = lambda frame: (frame, 0, 0)
    return pl.pallas_call(
        sort_kernel,
        grid=(frames,),
        in_specs=[
            pl.BlockSpec((1, 1, atoms), whole),
            pl.BlockSpec((1, atoms, LANES), whole),
            pl.BlockSpec((1, rows, atoms), whole),
        ],
        out_specs=[pl.BlockSpec((1, rows, atoms), whole), pl.BlockSpec((1, 1, atoms), whole)],
        out_shape=[
            jax.ShapeDtypeStruct((frames, rows, atoms), jnp.float32),
            jax.ShapeDtypeStruct((frames, 1, atoms), jnp.float32),
        ],
        compiler_params=pltpu.CompilerParams(vmem_limit_bytes=32 * 1024 * 1024),
        name="sort_atoms",
    )(key_row, key_col, payload)


def unsort_kernel(rank_ref, force_ref, out_ref):
    atoms = rank_ref.shape[2]
    value = force_ref[0]
    high, low = halves_of(value)
    left = value - high.astype(jnp.float32)
    third = (left - low.astype(jnp.float32)).astype(jnp.bfloat16)
    pieces = jnp.concatenate([high, low, third, jnp.zeros_like(high)], axis=0)
    rank = rank_ref[0].astype(jnp.int32)
    width = math.gcd(256, atoms)

    @pl.loop(0, atoms // width)
    def place(part):
        start = pl.multiple_of(part * width, width)
        spots = lax.broadcasted_iota(jnp.int32, (atoms, width), 0)
        lanes = pl.ds(start, width)
        here = rank_ref[0, :, lanes].astype(jnp.int32)
        chosen = jnp.where(here == spots, 1.0, 0.0).astype(jnp.bfloat16)
        moved = dot(pieces, chosen, NN)
        out_ref[0, :, lanes] = moved[0:8] + moved[8:16] + moved[16:24]


def unsort_forces(rank, forces):
    frames, rows, atoms = forces.shape
    whole = lambda frame: (frame, 0, 0)
    return pl.pallas_call(
        unsort_kernel,
        grid=(frames,),
        in_specs=[pl.BlockSpec((1, 1, atoms), whole), pl.BlockSpec((1, rows, atoms), whole)],
        out_specs=pl.BlockSpec((1, rows, atoms), whole),
        out_shape=jax.ShapeDtypeStruct((frames, rows, atoms), jnp.float32),
        compiler_params=pltpu.CompilerParams(vmem_limit_bytes=32 * 1024 * 1024),
        name="unsort_forces",
    )(rank, forces)


class Layout:
    def __init__(self, frames, length, atoms):
        self.rows = lax.axis_size("row")
        self.cols = lax.axis_size("col")
        self.frames = frames
        self.length = length
        self.atoms = atoms
        self.group = self.rows // frames
        self.half_cols = self.cols // 2
        self.block_rows = length // self.rows
        self.block_cols = length // self.cols
        self.slots = length // 2 // (self.group * self.half_cols)
        self.own = self.slots // 2
        self.slots_padded = max(8, self.slots)
        self.wave_rows = 2 * self.slots_padded
        self.lines = self.half_cols * self.block_cols + HALO
        self.lines_padded = -(-(self.lines + CHUNK - 1) // 8) * 8
        self.splits = self.group // 2
        self.blocks = atoms // LANES
        self.span = self.block_rows + HALO


def gather_kernel(lay, mine_ref, all_ref, local_sem, send_sem, recv_sem, pass_sem, took_sem):
    row = lax.axis_index("row")
    col = lax.axis_index("col")
    pair = col // 2
    side = col % 2
    half = col // lay.half_cols
    place = col % lay.half_cols
    hub = half == side
    pair_start = (2 * pair) % lay.half_cols

    def first_send(frame, member):
        target = frame * lay.group + member
        index = frame * lay.group + member
        return target, pltpu.make_async_remote_copy(
            src_ref=mine_ref.at[frame],
            dst_ref=all_ref.at[row, place],
            send_sem=send_sem.at[index],
            recv_sem=recv_sem.at[row, side],
            device_id=(target, 2 * pair + half),
            device_id_type=MESH,
        )

    def self_copy(frame):
        return pltpu.make_async_copy(mine_ref.at[frame], all_ref.at[row, place], local_sem)

    for frame in range(lay.frames):
        for member in range(lay.group):
            target, copy = first_send(frame, member)
            alone = (target == row) & hub

            @pl.when(jnp.logical_not(alone))
            def send():
                copy.start()

            @pl.when(alone)
            def keep():
                self_copy(frame).start()

    def second_send(source, part, other):
        spot = pair_start + part
        return pltpu.make_async_remote_copy(
            src_ref=all_ref.at[source, spot],
            dst_ref=all_ref.at[source, spot],
            send_sem=pass_sem.at[source, part, other - 1],
            recv_sem=took_sem.at[source, spot],
            device_id=(row, 2 * ((pair + other) % lay.half_cols) + side),
            device_id_type=MESH,
        )

    def arrival(source, spot, sem):
        return pltpu.make_async_remote_copy(
            src_ref=all_ref.at[source, spot],
            dst_ref=all_ref.at[source, spot],
            send_sem=send_sem.at[0],
            recv_sem=sem,
            device_id=(row, col),
            device_id_type=MESH,
        )

    @pl.when(hub)
    def forward():
        for source in range(lay.rows):
            for part in range(2):
                spot = pair_start + part
                alone = (source == row) & (part == side)

                @pl.when(jnp.logical_not(alone))
                def landed():
                    arrival(source, spot, recv_sem.at[source, part]).wait_recv()

                @pl.when(alone)
                def kept():
                    self_copy(row // lay.group).wait()

                for other in range(1, lay.half_cols):
                    second_send(source, part, other).start()

    for frame in range(lay.frames):
        for member in range(lay.group):
            target, copy = first_send(frame, member)

            @pl.when(jnp.logical_not((target == row) & hub))
            def sent():
                copy.wait_send()

    for spot in range(lay.half_cols):
        local = hub & (pair == side * (lay.half_cols // 2) + spot // 2)

        @pl.when(jnp.logical_not(local))
        def took():
            for source in range(lay.rows):
                arrival(source, spot, took_sem.at[source, spot]).wait_recv()

    @pl.when(hub)
    def passed():
        for source in range(lay.rows):
            for part in range(2):
                for other in range(1, lay.half_cols):
                    second_send(source, part, other).wait_send()


def gather_atoms(lay, mine):
    frames, rows, atoms = mine.shape
    dma = pltpu.SemaphoreType.DMA
    return pl.pallas_call(
        functools.partial(gather_kernel, lay),
        in_specs=[pl.BlockSpec(memory_space=pltpu.VMEM)],
        out_specs=pl.BlockSpec(memory_space=pltpu.VMEM),
        out_shape=jax.ShapeDtypeStruct((lay.rows, lay.half_cols, rows, atoms), jnp.float32),
        scratch_shapes=[
            dma,
            dma((lay.rows,)),
            dma((lay.rows, 2)),
            dma((lay.rows, 2, lay.half_cols - 1)),
            dma((lay.rows, lay.half_cols)),
        ],
        compiler_params=pltpu.CompilerParams(has_side_effects=True),
        name="gather_atoms",
    )(mine)


def return_kernel(lay, force_ref, out_ref, local_sem, send_sem, recv_sem):
    row = lax.axis_index("row")
    col = lax.axis_index("col")
    side = col % 2
    frame = row // lay.group
    index = (row % lay.group) * lay.half_cols + col // 2
    copies = []
    for source in range(lay.rows):
        for spot in range(lay.half_cols):
            owner = side * lay.half_cols + spot
            copies.append(
                (
                    (source == row) & (owner == col),
                    pltpu.make_async_remote_copy(
                        src_ref=force_ref.at[source, spot],
                        dst_ref=out_ref.at[frame, index],
                        send_sem=send_sem.at[source, spot],
                        recv_sem=recv_sem.at[frame, index],
                        device_id=(source, owner),
                        device_id_type=MESH,
                    ),
                    pltpu.make_async_copy(
                        force_ref.at[source, spot], out_ref.at[frame, index], local_sem
                    ),
                )
            )
    for alone, copy, local in copies:

        @pl.when(jnp.logical_not(alone))
        def send():
            copy.start()

        @pl.when(alone)
        def keep():
            local.start()

    for alone, copy, local in copies:

        @pl.when(jnp.logical_not(alone))
        def sent():
            copy.wait_send()

        @pl.when(alone)
        def kept():
            local.wait()

    half = col // lay.half_cols
    for from_frame in range(lay.frames):
        for member in range(lay.group):
            for pair in range(lay.half_cols):
                slot = member * lay.half_cols + pair
                alone = (from_frame * lay.group + member == row) & (2 * pair + half == col)

                @pl.when(jnp.logical_not(alone))
                def landed():
                    pltpu.make_async_remote_copy(
                        src_ref=out_ref.at[from_frame, slot],
                        dst_ref=out_ref.at[from_frame, slot],
                        send_sem=send_sem.at[0, 0],
                        recv_sem=recv_sem.at[from_frame, slot],
                        device_id=(row, col),
                        device_id_type=MESH,
                    ).wait_recv()


def return_forces(lay, forces):
    rows, half_cols = forces.shape[:2]
    members = lay.group * half_cols
    dma = pltpu.SemaphoreType.DMA
    return pl.pallas_call(
        functools.partial(return_kernel, lay),
        in_specs=[pl.BlockSpec(memory_space=pltpu.VMEM)],
        out_specs=pl.BlockSpec(memory_space=pltpu.VMEM),
        out_shape=jax.ShapeDtypeStruct((lay.frames, members) + forces.shape[2:], jnp.float32),
        scratch_shapes=[dma, dma((rows, half_cols)), dma((lay.frames, members))],
        compiler_params=pltpu.CompilerParams(has_side_effects=True),
        name="return_forces",
    )(forces)


def atom_block(lay, atoms_ref, waves_ref, block, with_slopes):
    lanes = pl.ds(pl.multiple_of(block * LANES, LANES), LANES)
    piece = atoms_ref[0, 0, :, lanes]
    cells = piece[0:3].astype(jnp.int32)
    values, slopes = spline_rows(piece[3:6])
    charge = piece[6:7]
    spots = lax.broadcasted_iota(jnp.int32, (lay.span, LANES), 0)
    kinds = [values, slopes] if with_slopes else [values]
    wide = dense(cells[0:1] + HALO - spots, [row_of(kind, 0) for kind in kinds])
    pad = jnp.zeros((LANES - lay.span, LANES), jnp.float32)
    wide = [jnp.concatenate([entry, pad], axis=0) for entry in wide]
    cosine, sine = phases(waves_ref[0] * cells[2:3] + waves_ref[1], lay.length)
    return cells, kinds, charge, wide, cosine, sine


def line_weights(cells, kinds, start, lay):
    lines = lax.broadcasted_iota(jnp.int32, (-(-CHUNK // 8) * 8, LANES), 0) + start
    return dense(cells[1:2] + HALO - lines, [row_of(kind, 1) for kind in kinds])


def spread_kernel(lay, starts_ref, turns_ref, atoms_ref, waves_ref, cos_ref, sin_ref, mesh_ref):
    part = pl.program_id(1)
    pencil = pl.program_id(0) * lay.half_cols + part

    @pl.when(part == 0)
    def clear():
        mesh_ref[...] = jnp.zeros_like(mesh_ref)

    @pl.loop(0, lay.blocks)
    def add_block(block):
        turns = turns_ref[pencil * lay.blocks + block]

        @pl.when(turns > 0)
        def live():
            cells, kinds, charge, wide, cosine, sine = atom_block(
                lay, atoms_ref, waves_ref, block, False
            )
            waves = wave_rows(cosine, sine, cos_ref, sin_ref, row_of(kinds[0], 2)) * charge
            high, low = halves_of(wide[0])
            right = jnp.concatenate(
                [
                    jnp.concatenate([high, high], axis=1),
                    jnp.concatenate([low, low], axis=1),
                ],
                axis=0,
            )
            start = starts_ref[pencil * lay.blocks + block]

            @pl.loop(0, turns)
            def add_lines(turn):
                line = start + turn * CHUNK
                (weights,) = line_weights(cells, kinds, line, lay)
                product = jnp.concatenate(
                    [weights[i : i + 1] * waves for i in range(CHUNK)], axis=0
                )
                high, low = halves_of(product)
                total = dot(jnp.concatenate([high, low], axis=1), right, NT)
                where = pl.ds(pl.multiple_of(line * lay.wave_rows, lay.wave_rows), CHUNK * lay.wave_rows)
                mesh_ref[0, where, :] += total[:, :LANES] + total[:, LANES:]


def atom_specs(lay):
    fixed = lambda row, part, *refs: (0, 0, 0)
    return [
        pl.BlockSpec((1, 1, 8, lay.atoms), lambda row, part, *refs: (row, part, 0, 0)),
        pl.BlockSpec((2, lay.wave_rows, LANES), fixed),
        pl.BlockSpec((6, lay.wave_rows, LANES), fixed),
        pl.BlockSpec((6, lay.wave_rows, LANES), fixed),
    ]


def spread(lay, starts, turns, atoms, waves, cosines, sines):
    size = lay.lines_padded * lay.wave_rows
    return pl.pallas_call(
        functools.partial(spread_kernel, lay),
        grid_spec=pltpu.PrefetchScalarGridSpec(
            num_scalar_prefetch=2,
            grid=(lay.rows, lay.half_cols),
            in_specs=atom_specs(lay),
            out_specs=pl.BlockSpec((1, size, LANES), lambda row, part, *refs: (row, 0, 0)),
        ),
        out_shape=jax.ShapeDtypeStruct((lay.rows, size, LANES), jnp.float32),
        compiler_params=pltpu.CompilerParams(vmem_limit_bytes=40 * 1024 * 1024),
        cost_estimate=pl.CostEstimate(flops=10**10, bytes_accessed=10**7, transcendentals=0),
        name="spread",
    )(starts, turns, atoms, waves, cosines, sines)


def sample_kernel(
    lay, starts_ref, turns_ref, atoms_ref, waves_ref, cos_ref, sin_ref, high_ref, low_ref, out_ref
):
    pencil = pl.program_id(0) * lay.half_cols + pl.program_id(1)

    @pl.loop(0, lay.blocks)
    def sample_block(block):
        turns = turns_ref[pencil * lay.blocks + block]
        out_ref[0, 0, :, pl.ds(block, 1), :] = jnp.zeros((3, 1, LANES), jnp.float32)

        @pl.when(turns > 0)
        def live():
            cells, kinds, charge, wide, cosine, sine = atom_block(
                lay, atoms_ref, waves_ref, block, True
            )
            third = wave_rows(cosine, sine, cos_ref, sin_ref, row_of(kinds[0], 2))
            third_slope = wave_rows(cosine, sine, cos_ref, sin_ref, row_of(kinds[1], 2))
            both = jnp.concatenate(wide, axis=1)
            high, low = halves_of(both)
            right = jnp.concatenate([high, high], axis=0)
            start = starts_ref[pencil * lay.blocks + block]

            def add_lines(turn, sums):
                line = start + turn * CHUNK
                weights, weight_slopes = line_weights(cells, kinds, line, lay)
                where = pl.ds(pl.multiple_of(line * lay.wave_rows, lay.wave_rows), CHUNK * lay.wave_rows)
                field_high = high_ref[0, where, :]
                field = jnp.concatenate([field_high, low_ref[0, where, :]], axis=1)
                found = dot(field, right) + dot(field_high, low)
                plain, sloped, across = sums
                for i in range(CHUNK):
                    lines = slice(i * lay.wave_rows, (i + 1) * lay.wave_rows)
                    value = found[lines, :LANES]
                    plain += value * weights[i : i + 1]
                    across += value * weight_slopes[i : i + 1]
                    sloped += found[lines, LANES:] * weights[i : i + 1]
                return plain, sloped, across

            nothing = jnp.zeros((lay.wave_rows, LANES), jnp.float32)
            plain, sloped, across = lax.fori_loop(0, turns, add_lines, (nothing, nothing, nothing))
            for dimension, value in enumerate((sloped * third, across * third, plain * third_slope)):
                total = -charge * jnp.sum(value, axis=0, keepdims=True)
                out_ref[0, 0, dimension, pl.ds(block, 1), :] = total


def sample(lay, starts, turns, atoms, waves, cosines, sines, high, low):
    size = lay.lines_padded * lay.wave_rows
    field = pl.BlockSpec((1, size, LANES), lambda row, part, *refs: (row, 0, 0))
    shape = (lay.rows, lay.half_cols, 3, lay.blocks, LANES)
    return pl.pallas_call(
        functools.partial(sample_kernel, lay),
        grid_spec=pltpu.PrefetchScalarGridSpec(
            num_scalar_prefetch=2,
            grid=(lay.rows, lay.half_cols),
            in_specs=atom_specs(lay) + [field, field],
            out_specs=pl.BlockSpec((1, 1) + shape[2:], lambda row, part, *refs: (row, part, 0, 0, 0)),
        ),
        out_shape=jax.ShapeDtypeStruct(shape, jnp.float32),
        compiler_params=pltpu.CompilerParams(vmem_limit_bytes=40 * 1024 * 1024),
        cost_estimate=pl.CostEstimate(flops=10**10, bytes_accessed=10**7, transcendentals=0),
        name="sample",
    )(starts, turns, atoms, waves, cosines, sines, high, low)


def transform_kernel(
    lay,
    mesh_ref,
    green_ref,
    first_high,
    first_low,
    second_high,
    second_low,
    back_high,
    back_low,
    last_high,
    last_low,
    out_high,
    out_low,
    field_ref,
    mine_ref,
    send_ref,
    recv_ref,
    home_ref,
    extra_ref,
    send_sem,
    recv_sem,
    back_sem,
    home_sem,
):
    row = lax.axis_index("row")
    col = lax.axis_index("col")
    side = col % 2
    partner = (row, col + 1 - 2 * side)
    lines, length, own, padded = lay.lines, lay.length, lay.own, lay.slots_padded
    inner = lines - HALO

    def three(high, low, table_high, table_low):
        return dot(high, table_high) + dot(low, table_high) + dot(high, table_low)

    def push(index):
        return pltpu.make_async_remote_copy(
            src_ref=send_ref.at[index],
            dst_ref=recv_ref.at[index],
            send_sem=send_sem.at[index],
            recv_sem=recv_sem.at[index],
            device_id=partner,
            device_id_type=MESH,
        )

    def push_back(index):
        return pltpu.make_async_remote_copy(
            src_ref=send_ref.at[index],
            dst_ref=home_ref.at[index],
            send_sem=back_sem.at[index],
            recv_sem=home_sem.at[index],
            device_id=partner,
            device_id_type=MESH,
        )

    def forward(slot):
        rows = [
            jnp.concatenate(
                [mesh_ref[r, pl.ds(start, lines, stride=lay.wave_rows), :] for r in range(lay.rows)],
                axis=1,
            )
            for start in (slot, padded + slot)
        ]
        high, low = halves_of(jnp.concatenate(rows, axis=0))
        found = three(high, low, first_high[...], first_low[...])
        upper, lower = found[:lines], found[lines:]
        return upper[:, :length], upper[:, length:], lower[:, :length], lower[:, length:]

    for base, target in ((0, send_ref), (own, mine_ref)):
        away = base == 0

        @pl.loop(0, own)
        def first_pass(i):
            real_cos, real_sin, imag_cos, imag_sin = forward(base + i)

            @pl.when(i == 0)
            def mirrored():
                target[own, 0] = real_cos - imag_sin
                target[own, 1] = -imag_cos - real_sin

            target[i, 0] = real_cos + imag_sin
            target[i, 1] = imag_cos - real_sin
            if away:

                @pl.when(i == 0)
                def start_mirrored():
                    push(own).start()

                push(i).start()

    @pl.loop(0, own + 1)
    def sent(i):
        push(i).wait_send()

    number = message_number(lay, row, col)

    def spectrum(index):
        mine, other = mine_ref[index], recv_ref[index]
        parts = []
        for part in range(2):
            a, b = mine[part], other[part]
            parts.append(
                jnp.concatenate(
                    [
                        a[HALO:inner],
                        a[inner:] + b[:HALO],
                        b[HALO:inner],
                        b[inner:] + a[:HALO],
                    ],
                    axis=0,
                )
            )
        high, low = halves_of(jnp.concatenate(parts, axis=1))
        found = (
            dot(second_high[...], high) + dot(second_high[...], low) + dot(second_low[...], high)
        )
        cos_part, sin_part = found[:length], found[length:]
        real = cos_part[:, :length] + sin_part[:, length:]
        imag = cos_part[:, length:] - sin_part[:, :length]
        blocks = [green_ref[lax.rem(r + number, lay.rows), index] for r in range(lay.rows)]
        green = jnp.concatenate(blocks, axis=0)
        return real * green, imag * green

    push(own).wait_recv()
    extra_ref[0], extra_ref[1] = spectrum(own)

    @pl.loop(0, own)
    def second_pass(i):
        push(i).wait_recv()
        real, imag = spectrum(i)
        first = jnp.where(i == 0, 1.0, 0.0)
        real += first * extra_ref[0]
        imag += first * extra_ref[1]
        high, low = halves_of(jnp.concatenate([real, imag], axis=1))
        found = dot(back_high[...], high) + dot(back_high[...], low) + dot(back_low[...], high)
        cos_part, sin_part = found[: 2 * lines], found[2 * lines :]
        real = cos_part[:, :length] - sin_part[:, length:]
        imag = cos_part[:, length:] + sin_part[:, :length]
        mine_ref[i, 0] = real[:lines]
        mine_ref[i, 1] = imag[:lines]
        send_ref[i, 0] = real[lines:]
        send_ref[i, 1] = imag[lines:]
        push_back(i).start()

    cleared = 0 if lay.slots < padded else lines * lay.wave_rows
    total_rows = lay.lines_padded * lay.wave_rows
    for r in range(lay.rows):
        field_ref[r, pl.ds(cleared, total_rows - cleared), :] = jnp.zeros(
            (total_rows - cleared, LANES), jnp.float32
        )

    def last(local, planes_ref, i):
        high, low = halves_of(jnp.concatenate([planes_ref[i, 0], planes_ref[i, 1]], axis=1))
        found = three(high, low, last_high[...], last_low[...])
        for part in range(2):
            for r in range(lay.rows):
                lanes = (part * lay.rows + r) * LANES
                where = pl.ds(part * padded + local, lines, stride=lay.wave_rows)
                field_ref[r, where, :] = found[:, lanes : lanes + LANES]

    @pl.loop(0, own)
    def last_mine(i):
        last(own + i, mine_ref, i)

    @pl.loop(0, own)
    def last_home(i):
        push_back(i).wait_recv()
        last(i, home_ref, i)

    @pl.loop(0, lay.lines_padded)
    def split(line):
        where = pl.ds(pl.multiple_of(line * lay.wave_rows, lay.wave_rows), lay.wave_rows)
        for r in range(lay.rows):
            out_high[r, where, :], out_low[r, where, :] = halves_of(field_ref[r, where, :])

    @pl.loop(0, own)
    def returned(i):
        push_back(i).wait_send()


def message_number(lay, row, col):
    member = lax.rem(row, lay.group)
    frame = row // lay.group
    return (lax.rem(col, 2) * lay.frames + frame) * lay.splits + lax.rem(member, lay.splits)


def transform(lay, mesh, green, tables):
    dma = pltpu.SemaphoreType.DMA
    plane = (2, lay.lines, lay.length)
    vmem = pl.BlockSpec(memory_space=pltpu.VMEM)
    out = jax.ShapeDtypeStruct(mesh.shape, jnp.bfloat16)
    return pl.pallas_call(
        functools.partial(transform_kernel, lay),
        in_specs=[vmem] * (2 + len(tables)),
        out_specs=[vmem, vmem],
        out_shape=[out, out],
        scratch_shapes=[
            pltpu.VMEM(mesh.shape, jnp.float32),
            pltpu.VMEM((lay.own + 1,) + plane, jnp.float32),
            pltpu.VMEM((lay.own + 1,) + plane, jnp.float32),
            pltpu.VMEM((lay.own + 1,) + plane, jnp.float32),
            pltpu.VMEM((lay.own,) + plane, jnp.float32),
            pltpu.VMEM((2, lay.length, lay.length), jnp.float32),
            dma((lay.own + 1,)),
            dma((lay.own + 1,)),
            dma((lay.own,)),
            dma((lay.own,)),
        ],
        compiler_params=pltpu.CompilerParams(
            has_side_effects=True, vmem_limit_bytes=62 * 1024 * 1024
        ),
        cost_estimate=pl.CostEstimate(flops=10**10, bytes_accessed=10**7, transcendentals=0),
        name="transform",
    )(mesh, green, *tables)


def table_halves(value):
    leading = lax.reduce_precision(value, exponent_bits=8, mantissa_bits=7)
    return leading.astype(jnp.bfloat16), (value - leading).astype(jnp.bfloat16)


def make_tables(lay, side):
    length, half = lay.length, lay.half_cols * lay.block_cols
    waves = jnp.arange(length, dtype=jnp.int32)
    spots = jnp.arange(LANES, dtype=jnp.int32)
    blocks = jnp.arange(lay.rows, dtype=jnp.int32)
    zero = lax.optimization_barrier(jnp.int32(0))
    across = (blocks[:, None] * lay.block_rows + spots[None, :] - HALO).reshape(-1) + length + zero
    valid = jnp.tile(spots < lay.span, lay.rows)
    cosine, sine = phases(across[:, None] * waves[None, :], length)
    keep = valid[:, None]
    first = jnp.where(keep, jnp.concatenate([cosine, sine], axis=1), 0.0)
    cosine, sine = phases(across[None, :] * waves[:, None], length)
    top = jnp.concatenate([cosine, sine], axis=1)
    bottom = jnp.concatenate([-sine, cosine], axis=1)
    last = jnp.where(jnp.tile(valid, 2)[None, :], jnp.concatenate([top, bottom], axis=0), 0.0)
    along = waves + half * side
    second = jnp.concatenate(phases(waves[:, None] * along[None, :], length), axis=0)
    near = jnp.arange(lay.lines, dtype=jnp.int32) - HALO + length
    both = jnp.concatenate([near + half * side, near + half * (1 - side)])
    back = jnp.concatenate(phases(both[:, None] * waves[None, :], length), axis=0)
    tables = []
    for table in (first, second, back, last):
        tables.extend(table_halves(table))
    return tables


def make_waves(lay, row, col, side):
    length = lay.length
    member = row % lay.group
    source = 2 * (col // 2) + member // lay.splits
    split = member % lay.splits
    start = lay.block_cols * source + jnp.where(source >= lay.half_cols, 1, 0) + split * lay.slots
    index = jnp.arange(lay.slots_padded, dtype=jnp.int32)
    slot = jnp.where(index < lay.own, (1 - side) * lay.own, side * lay.own) + index % lay.own
    special = (source == 0) & (split == 0) & (slot == 0)
    waves = jnp.concatenate([start + slot, jnp.where(special, length // 2, start + slot)])
    turns = jnp.concatenate([jnp.zeros_like(slot), jnp.where(special, 0, length // 4)])
    live = jnp.tile(index < lay.slots, 2)[None, :, None]
    offsets = jnp.arange(6, dtype=jnp.int32)
    cosine, sine = phases(offsets[:, None] * waves[None, :], length)
    shape = (6, lay.wave_rows, LANES)
    cosines = jnp.broadcast_to(jnp.where(live, cosine[:, :, None], 0.0), shape)
    sines = jnp.broadcast_to(jnp.where(live, sine[:, :, None], 0.0), shape)
    both = jnp.broadcast_to(jnp.stack([waves, turns])[:, :, None], (2, lay.wave_rows, LANES))
    return both, cosines, sines


def share_green(lay, influence, row, col):
    length = lay.length
    rows, cols = lay.rows, lay.cols
    scale = 1.0 / float(length) ** 3
    used = lay.block_cols // 2
    offset = jnp.where(col >= lay.half_cols, 1, 0)
    middle = lax.ppermute(influence[:, 0, :], "col", [(lay.half_cols, 0)])
    block = lax.dynamic_slice_in_dim(influence, offset, used, axis=1).transpose(1, 0, 2)
    block = block.reshape(lay.splits, 2, lay.own, lay.block_rows, length)
    special = col == 0
    zeroth = block[0, 0, 0]
    extra = jnp.where(special, (0.5 * scale) * (zeroth - middle), 0.0)
    zeroth = jnp.where(special, (0.5 * scale) * (zeroth + middle), (2.0 * scale) * zeroth)
    block = jnp.concatenate([(2.0 * scale) * block, jnp.zeros_like(block[:, :, :1])], axis=2)
    block = block.at[0, 0, 0].set(zeroth).at[0, 0, lay.own].set(extra)
    block = block.reshape((2 * lay.splits,) + block.shape[2:])
    messages = []
    for number in range(rows):
        message = (number - row) % rows
        split = message % lay.splits
        side = message // (lay.frames * lay.splits)
        sent = lax.dynamic_index_in_dim(block, split * 2 + side, keepdims=False)
        pairs = []
        for r in range(rows):
            at = (number - r) % rows
            to_split, rest = at % lay.splits, at // lay.splits
            to_frame, to_side = rest % lay.frames, rest // lay.frames
            for c in range(cols):
                to_row = to_frame * lay.group + (c % 2) * lay.splits + to_split
                pairs.append((r * cols + c, to_row * cols + 2 * (c // 2) + to_side))
        messages.append(lax.ppermute(sent, ("row", "col"), pairs))
    return jnp.stack(messages)


def shards(cell_index, fraction, charge, atom_count, influence):
    frames, unused, atoms = fraction.shape
    lay = Layout(frames, influence.shape[2], atoms)
    row = lax.axis_index("row")
    col = lax.axis_index("col")
    side = col % 2
    green = share_green(lay, influence, row, col)
    tables = make_tables(lay, side)
    waves, cosines, sines = make_waves(lay, row, col, side)

    slot_ids = jnp.arange(atoms, dtype=jnp.int32)
    alive = slot_ids[None, :] < atom_count
    charges = jnp.where(alive, charge, 0.0)
    origin = jnp.stack([row * lay.block_rows, (col // lay.half_cols) * lay.half_cols * lay.block_cols, 0])
    cells = cell_index - origin[None, :, None]
    payload = jnp.concatenate(
        [
            cells.astype(jnp.float32),
            fraction,
            charges[:, None, :],
            alive[:, None, :].astype(jnp.float32),
        ],
        axis=1,
    )
    key = (jnp.where(alive, cells[:, 1], lay.length) * atoms + slot_ids[None, :]).astype(jnp.float32)
    key_col = jnp.broadcast_to(key[:, :, None], (frames, atoms, LANES))
    sorted_atoms, rank = sort_atoms(key[:, None, :], key_col, payload)
    shared = gather_atoms(lay, sorted_atoms)

    lines = shared[:, :, 1, :].reshape(lay.rows * lay.half_cols * lay.blocks, LANES)
    lives = shared[:, :, 7, :].reshape(lines.shape) > 0.5
    lowest = jnp.min(jnp.where(lives, lines, 1024.0), axis=1).astype(jnp.int32)
    highest = jnp.max(jnp.where(lives, lines, -1024.0), axis=1).astype(jnp.int32)
    starts = lowest + HALO - 5
    turns = jnp.where(highest >= lowest, (highest - lowest + 6 + CHUNK - 1) // CHUNK, 0)

    mesh = spread(lay, starts, turns, shared, waves, cosines, sines)
    high, low = transform(lay, mesh, green, tables)
    partial = sample(lay, starts, turns, shared, waves, cosines, sines, high, low)
    returned = return_forces(lay, partial)
    forces = jnp.sum(returned, axis=1).reshape(frames, 3, atoms)
    forces = jnp.pad(forces, ((0, 0), (0, 5), (0, 0)))
    return unsort_forces(rank, forces)[:, :3]


def solution(mesh):
    placed = (
        P(None, None, ("row", "col")),
        P(None, None, ("row", "col")),
        P(None, ("row", "col")),
        P(None, ("row", "col")),
        P("row", "col", None),
    )
    return jax.shard_map(
        shards, mesh=mesh, in_specs=placed, out_specs=P(None, None, ("row", "col")), check_vma=False
    )
```

```python
import functools
import math

import jax
import jax.numpy as jnp
from jax import lax
from jax.experimental import pallas as pl
from jax.experimental.pallas import tpu as pltpu
from jax.sharding import PartitionSpec as P


MESH = pl.DeviceIdType.MESH
LANES = 128
CHUNK = 9
PACK = 4
HALO = 8
NT = (((1,), (1,)), ((), ()))
NN = (((1,), (0,)), ((), ()))


def dot(left, right, form=NN):
    return lax.dot_general(left, right, form, preferred_element_type=jnp.float32)


def halves_of(value):
    high = value.astype(jnp.bfloat16)
    return high, (value - high.astype(jnp.float32)).astype(jnp.bfloat16)


def spline_rows(fraction):
    nothing = jnp.zeros_like(fraction)
    levels = [fraction, 1.0 - fraction]
    slopes = levels
    for degree in range(3, 7):
        padded = levels + [nothing]
        following = []
        for offset in range(degree):
            beneath = padded[offset - 1] if offset > 0 else nothing
            following.append(
                ((fraction + offset) * padded[offset] + (degree - fraction - offset) * beneath)
                * (1.0 / (degree - 1))
            )
        if degree == 6:
            slopes = [
                padded[offset] - (padded[offset - 1] if offset > 0 else nothing)
                for offset in range(6)
            ]
        levels = following
    return levels, slopes


def dense(distance, lists):
    results = [jnp.zeros(distance.shape, jnp.float32) for _ in lists]
    for offset in range(6):
        hit = distance == offset
        results = [jnp.where(hit, rows[offset], result) for rows, result in zip(lists, results)]
    return results


def row_of(lists, dimension):
    return [entry[dimension : dimension + 1, :] for entry in lists]


def phases(product, length):
    half = length // 2
    moved = product + half
    if length & (length - 1):
        turned = lax.rem(moved, length) - half
    else:
        turned = (moved & (length - 1)) - half
    angle = turned.astype(jnp.float32) * (2.0 * math.pi / length / 4.0)
    square = angle * angle
    sine = angle * (
        1.0
        + square
        * (-1.0 / 6 + square * (1.0 / 120 + square * (-1.0 / 5040 + square * (1.0 / 362880))))
    )
    cosine = 1.0 + square * (
        -0.5
        + square
        * (1.0 / 24 + square * (-1.0 / 720 + square * (1.0 / 40320 - square * (1.0 / 3628800))))
    )
    for _ in range(2):
        sine, cosine = 2.0 * sine * cosine, 1.0 - 2.0 * sine * sine
    return cosine, sine


def wave_rows(cosine, sine, cos_ref, sin_ref, rows):
    copies = cosine.shape[1] // LANES

    def wide(ref, offset):
        return jnp.concatenate([ref[offset]] * copies, axis=1) * rows[offset]

    even, odd = wide(cos_ref, 0), wide(sin_ref, 0)
    for offset in range(1, 6):
        even += wide(cos_ref, offset)
        odd += wide(sin_ref, offset)
    return cosine * even + sine * odd


def sort_kernel(key_row_ref, key_col_ref, payload_ref, sorted_ref, rank_ref):
    atoms = key_row_ref.shape[2]

    @pl.loop(0, atoms // LANES)
    def count(part):
        lanes = pl.ds(pl.multiple_of(part * LANES, LANES), LANES)
        below = key_col_ref[0] < key_row_ref[0, :, lanes]
        rank_ref[0, :, lanes] = jnp.sum(jnp.where(below, 1.0, 0.0), axis=0, keepdims=True)

    value = payload_ref[0]
    first, rest = halves_of(value)
    left = value - first.astype(jnp.float32)
    third = (left - rest.astype(jnp.float32)).astype(jnp.bfloat16)
    pieces = jnp.concatenate([first, rest, third, jnp.zeros_like(first)], axis=0)
    rank = rank_ref[0].astype(jnp.int32)
    width = math.gcd(256, atoms)

    @pl.loop(0, atoms // width)
    def place(part):
        start = pl.multiple_of(part * width, width)
        spots = lax.broadcasted_iota(jnp.int32, (width, atoms), 0) + start
        chosen = jnp.where(rank == spots, 1.0, 0.0).astype(jnp.bfloat16)
        moved = dot(pieces, chosen, NT)
        sorted_ref[0, :, pl.ds(start, width)] = moved[0:8] + moved[8:16] + moved[16:24]


def sort_atoms(key_row, key_col, payload):
    frames, rows, atoms = payload.shape
    whole = lambda frame: (frame, 0, 0)
    return pl.pallas_call(
        sort_kernel,
        grid=(frames,),
        in_specs=[
            pl.BlockSpec((1, 1, atoms), whole),
            pl.BlockSpec((1, atoms, LANES), whole),
            pl.BlockSpec((1, rows, atoms), whole),
        ],
        out_specs=[pl.BlockSpec((1, rows, atoms), whole), pl.BlockSpec((1, 1, atoms), whole)],
        out_shape=[
            jax.ShapeDtypeStruct((frames, rows, atoms), jnp.float32),
            jax.ShapeDtypeStruct((frames, 1, atoms), jnp.float32),
        ],
        compiler_params=pltpu.CompilerParams(vmem_limit_bytes=32 * 1024 * 1024),
        name="sort_atoms",
    )(key_row, key_col, payload)


def unsort_kernel(rank_ref, force_ref, out_ref):
    atoms = rank_ref.shape[2]
    value = force_ref[0]
    high, low = halves_of(value)
    left = value - high.astype(jnp.float32)
    third = (left - low.astype(jnp.float32)).astype(jnp.bfloat16)
    pieces = jnp.concatenate([high, low, third, jnp.zeros_like(high)], axis=0)
    rank = rank_ref[0].astype(jnp.int32)
    width = math.gcd(256, atoms)

    @pl.loop(0, atoms // width)
    def place(part):
        start = pl.multiple_of(part * width, width)
        spots = lax.broadcasted_iota(jnp.int32, (atoms, width), 0)
        lanes = pl.ds(start, width)
        here = rank_ref[0, :, lanes].astype(jnp.int32)
        chosen = jnp.where(here == spots, 1.0, 0.0).astype(jnp.bfloat16)
        moved = dot(pieces, chosen, NN)
        out_ref[0, :, lanes] = moved[0:8] + moved[8:16] + moved[16:24]


def unsort_forces(rank, forces):
    frames, rows, atoms = forces.shape
    whole = lambda frame: (frame, 0, 0)
    return pl.pallas_call(
        unsort_kernel,
        grid=(frames,),
        in_specs=[pl.BlockSpec((1, 1, atoms), whole), pl.BlockSpec((1, rows, atoms), whole)],
        out_specs=pl.BlockSpec((1, rows, atoms), whole),
        out_shape=jax.ShapeDtypeStruct((frames, rows, atoms), jnp.float32),
        compiler_params=pltpu.CompilerParams(vmem_limit_bytes=32 * 1024 * 1024),
        name="unsort_forces",
    )(rank, forces)


class Layout:
    def __init__(self, frames, length, atoms):
        self.rows = lax.axis_size("row")
        self.cols = lax.axis_size("col")
        self.frames = frames
        self.length = length
        self.atoms = atoms
        self.group = self.rows // frames
        self.half_cols = self.cols // 2
        self.block_rows = length // self.rows
        self.block_cols = length // self.cols
        self.slots = length // 2 // (self.group * self.half_cols)
        self.own = self.slots // 2
        self.slots_padded = max(8, self.slots)
        self.wave_rows = 2 * self.slots_padded
        self.stride = self.wave_rows + 1
        self.lines = self.half_cols * self.block_cols + HALO
        self.lines_padded = -(-(self.lines + CHUNK - 1) // 8) * 8
        self.splits = self.group // 2
        self.blocks = atoms // LANES
        self.span = self.block_rows + HALO
        self.pack = math.gcd(PACK, self.blocks)


def gather_kernel(lay, mine_ref, all_ref, local_sem, send_sem, recv_sem, pass_sem, took_sem):
    row = lax.axis_index("row")
    col = lax.axis_index("col")
    pair = col // 2
    side = col % 2
    half = col // lay.half_cols
    place = col % lay.half_cols
    hub = half == side
    pair_start = (2 * pair) % lay.half_cols

    def first_send(frame, member):
        target = frame * lay.group + member
        index = frame * lay.group + member
        return target, pltpu.make_async_remote_copy(
            src_ref=mine_ref.at[frame],
            dst_ref=all_ref.at[row, place],
            send_sem=send_sem.at[index],
            recv_sem=recv_sem.at[row, side],
            device_id=(target, 2 * pair + half),
            device_id_type=MESH,
        )

    def self_copy(frame):
        return pltpu.make_async_copy(mine_ref.at[frame], all_ref.at[row, place], local_sem)

    for frame in range(lay.frames):
        for member in range(lay.group):
            target, copy = first_send(frame, member)
            alone = (target == row) & hub

            @pl.when(jnp.logical_not(alone))
            def send():
                copy.start()

            @pl.when(alone)
            def keep():
                self_copy(frame).start()

    def second_send(source, part, other):
        spot = pair_start + part
        return pltpu.make_async_remote_copy(
            src_ref=all_ref.at[source, spot],
            dst_ref=all_ref.at[source, spot],
            send_sem=pass_sem.at[source, part, other - 1],
            recv_sem=took_sem.at[source, spot],
            device_id=(row, 2 * ((pair + other) % lay.half_cols) + side),
            device_id_type=MESH,
        )

    def arrival(source, spot, sem):
        return pltpu.make_async_remote_copy(
            src_ref=all_ref.at[source, spot],
            dst_ref=all_ref.at[source, spot],
            send_sem=send_sem.at[0],
            recv_sem=sem,
            device_id=(row, col),
            device_id_type=MESH,
        )

    @pl.when(hub)
    def forward():
        for source in range(lay.rows):
            for part in range(2):
                spot = pair_start + part
                alone = (source == row) & (part == side)

                @pl.when(jnp.logical_not(alone))
                def landed():
                    arrival(source, spot, recv_sem.at[source, part]).wait_recv()

                @pl.when(alone)
                def kept():
                    self_copy(row // lay.group).wait()

                for other in range(1, lay.half_cols):
                    second_send(source, part, other).start()

    for frame in range(lay.frames):
        for member in range(lay.group):
            target, copy = first_send(frame, member)

            @pl.when(jnp.logical_not((target == row) & hub))
            def sent():
                copy.wait_send()

    for spot in range(lay.half_cols):
        local = hub & (pair == side * (lay.half_cols // 2) + spot // 2)

        @pl.when(jnp.logical_not(local))
        def took():
            for source in range(lay.rows):
                arrival(source, spot, took_sem.at[source, spot]).wait_recv()

    @pl.when(hub)
    def passed():
        for source in range(lay.rows):
            for part in range(2):
                for other in range(1, lay.half_cols):
                    second_send(source, part, other).wait_send()


def gather_atoms(lay, mine):
    _, rows, atoms = mine.shape
    dma = pltpu.SemaphoreType.DMA
    return pl.pallas_call(
        functools.partial(gather_kernel, lay),
        in_specs=[pl.BlockSpec(memory_space=pltpu.VMEM)],
        out_specs=pl.BlockSpec(memory_space=pltpu.VMEM),
        out_shape=jax.ShapeDtypeStruct((lay.rows, lay.half_cols, rows, atoms), jnp.float32),
        scratch_shapes=[
            dma,
            dma((lay.rows,)),
            dma((lay.rows, 2)),
            dma((lay.rows, 2, lay.half_cols - 1)),
            dma((lay.rows, lay.half_cols)),
        ],
        compiler_params=pltpu.CompilerParams(has_side_effects=True),
        name="gather_atoms",
    )(mine)


def return_kernel(lay, force_ref, out_ref, local_sem, send_sem, recv_sem):
    row = lax.axis_index("row")
    col = lax.axis_index("col")
    side = col % 2
    frame = row // lay.group
    index = (row % lay.group) * lay.half_cols + col // 2
    copies = []
    for source in range(lay.rows):
        for spot in range(lay.half_cols):
            owner = side * lay.half_cols + spot
            copies.append(
                (
                    (source == row) & (owner == col),
                    pltpu.make_async_remote_copy(
                        src_ref=force_ref.at[source, spot],
                        dst_ref=out_ref.at[frame, index],
                        send_sem=send_sem.at[source, spot],
                        recv_sem=recv_sem.at[frame, index],
                        device_id=(source, owner),
                        device_id_type=MESH,
                    ),
                    pltpu.make_async_copy(
                        force_ref.at[source, spot], out_ref.at[frame, index], local_sem
                    ),
                )
            )
    for alone, copy, local in copies:

        @pl.when(jnp.logical_not(alone))
        def send():
            copy.start()

        @pl.when(alone)
        def keep():
            local.start()

    for alone, copy, local in copies:

        @pl.when(jnp.logical_not(alone))
        def sent():
            copy.wait_send()

        @pl.when(alone)
        def kept():
            local.wait()

    half = col // lay.half_cols
    for from_frame in range(lay.frames):
        for member in range(lay.group):
            for pair in range(lay.half_cols):
                slot = member * lay.half_cols + pair
                alone = (from_frame * lay.group + member == row) & (2 * pair + half == col)

                @pl.when(jnp.logical_not(alone))
                def landed():
                    pltpu.make_async_remote_copy(
                        src_ref=out_ref.at[from_frame, slot],
                        dst_ref=out_ref.at[from_frame, slot],
                        send_sem=send_sem.at[0, 0],
                        recv_sem=recv_sem.at[from_frame, slot],
                        device_id=(row, col),
                        device_id_type=MESH,
                    ).wait_recv()


def return_forces(lay, forces):
    rows, half_cols = forces.shape[:2]
    members = lay.group * half_cols
    dma = pltpu.SemaphoreType.DMA
    return pl.pallas_call(
        functools.partial(return_kernel, lay),
        in_specs=[pl.BlockSpec(memory_space=pltpu.VMEM)],
        out_specs=pl.BlockSpec(memory_space=pltpu.VMEM),
        out_shape=jax.ShapeDtypeStruct((lay.frames, members) + forces.shape[2:], jnp.float32),
        scratch_shapes=[dma, dma((rows, half_cols)), dma((lay.frames, members))],
        compiler_params=pltpu.CompilerParams(has_side_effects=True),
        name="return_forces",
    )(forces)


def atom_group(lay, atoms_ref, waves_ref, group, with_slopes):
    width = lay.pack * LANES
    lanes = pl.ds(pl.multiple_of(group * width, width), width)
    piece = atoms_ref[0, 0, :, lanes]
    cells = piece[0:3].astype(jnp.int32)
    values, slopes = spline_rows(piece[3:6])
    charge = piece[6:7]
    spots = lax.broadcasted_iota(jnp.int32, (lay.span, width), 0)
    kinds = [values, slopes] if with_slopes else [values]
    wide = dense(cells[0:1] + HALO - spots, [row_of(kind, 0) for kind in kinds])
    pad = jnp.zeros((LANES - lay.span, width), jnp.float32)
    wide = [jnp.concatenate([entry, pad], axis=0) for entry in wide]
    turned = jnp.concatenate([waves_ref[0]] * lay.pack, axis=1) * cells[2:3]
    turned += jnp.concatenate([waves_ref[1]] * lay.pack, axis=1)
    cosine, sine = phases(turned, lay.length)
    return cells, kinds, charge, wide, cosine, sine


def line_weights(cells, kinds, starts):
    lines = lax.broadcasted_iota(jnp.int32, (-(-CHUNK // 8) * 8, LANES), 0)
    lines = jnp.concatenate([lines + start for start in starts], axis=1)
    return dense(cells[1:2] + HALO - lines, [row_of(kind, 1) for kind in kinds])


def lanes_of(block):
    return slice(block * LANES, (block + 1) * LANES)


def pick(kinds, block):
    return [[row[:, lanes_of(block)] for row in kind] for kind in kinds]


def rows_at(lay, line):
    return pl.ds(pl.multiple_of(line * lay.wave_rows, lay.wave_rows), CHUNK * lay.wave_rows)


def spread_kernel(lay, starts_ref, turns_ref, atoms_ref, waves_ref, cos_ref, sin_ref, mesh_ref):
    part = pl.program_id(1)
    pencil = pl.program_id(0) * lay.half_cols + part

    @pl.when(part == 0)
    def clear():
        mesh_ref[...] = jnp.zeros_like(mesh_ref)

    @pl.loop(0, lay.blocks // lay.pack)
    def add_group(group):
        base = pencil * lay.blocks + group * lay.pack

        @pl.when(turns_ref[base] > 0)
        def live():
            cells, kinds, charge, wide, cosine, sine = atom_group(
                lay, atoms_ref, waves_ref, group, False
            )
            waves = wave_rows(cosine, sine, cos_ref, sin_ref, row_of(kinds[0], 2)) * charge
            starts = [starts_ref[base + block] for block in range(lay.pack)]
            (weights,) = line_weights(cells, kinds, starts)
            rights = []
            for block in range(lay.pack):
                high, low = halves_of(wide[0][:, lanes_of(block)])
                rights.append(
                    jnp.concatenate(
                        [
                            jnp.concatenate([high, high], axis=1),
                            jnp.concatenate([low, low], axis=1),
                        ],
                        axis=0,
                    )
                )

            def total_of(weights, block):
                wave = waves[:, lanes_of(block)]
                product = jnp.concatenate([weights[i : i + 1] * wave for i in range(CHUNK)], axis=0)
                high, low = halves_of(product)
                total = dot(jnp.concatenate([high, low], axis=1), rights[block], NT)
                return total[:, :LANES] + total[:, LANES:]

            totals = [total_of(weights[:, lanes_of(block)], block) for block in range(lay.pack)]

            def add(line, total):
                for i in range(CHUNK):
                    part = total[i * lay.wave_rows : (i + 1) * lay.wave_rows]
                    mesh_ref[0, pl.ds((line + i) * lay.stride, lay.wave_rows), :] += part

            for block in range(lay.pack):
                add(starts[block], totals[block])
            for block in range(lay.pack):

                @pl.loop(1, turns_ref[base + block])
                def more(turn):
                    line = starts[block] + turn * CHUNK
                    lanes = lanes_of(block)
                    (weights,) = line_weights(cells[:, lanes], pick(kinds, block), [line])
                    add(line, total_of(weights, block))


def atom_specs(lay):
    fixed = lambda row, part, *refs: (0, 0, 0)
    return [
        pl.BlockSpec((1, 1, 8, lay.atoms), lambda row, part, *refs: (row, part, 0, 0)),
        pl.BlockSpec((2, lay.wave_rows, LANES), fixed),
        pl.BlockSpec((6, lay.wave_rows, LANES), fixed),
        pl.BlockSpec((6, lay.wave_rows, LANES), fixed),
    ]


def spread(lay, starts, turns, atoms, waves, cosines, sines):
    size = -(-lay.lines_padded * lay.stride // 8) * 8
    return pl.pallas_call(
        functools.partial(spread_kernel, lay),
        grid_spec=pltpu.PrefetchScalarGridSpec(
            num_scalar_prefetch=2,
            grid=(lay.rows, lay.half_cols),
            in_specs=atom_specs(lay),
            out_specs=pl.BlockSpec((1, size, LANES), lambda row, part, *refs: (row, 0, 0)),
        ),
        out_shape=jax.ShapeDtypeStruct((lay.rows, size, LANES), jnp.float32),
        compiler_params=pltpu.CompilerParams(vmem_limit_bytes=40 * 1024 * 1024),
        cost_estimate=pl.CostEstimate(flops=10**10, bytes_accessed=10**7, transcendentals=0),
        name="spread",
    )(starts, turns, atoms, waves, cosines, sines)


def sample_kernel(
    lay, starts_ref, turns_ref, atoms_ref, waves_ref, cos_ref, sin_ref, high_ref, low_ref, out_ref
):
    pencil = pl.program_id(0) * lay.half_cols + pl.program_id(1)

    @pl.loop(0, lay.blocks // lay.pack)
    def sample_group(group):
        base = pencil * lay.blocks + group * lay.pack
        first = group * lay.pack

        @pl.when(turns_ref[base] == 0)
        def idle():
            for block in range(lay.pack):
                out_ref[0, 0, :, pl.ds(first + block, 1), :] = jnp.zeros((3, 1, LANES), jnp.float32)

        @pl.when(turns_ref[base] > 0)
        def live():
            cells, kinds, charge, wide, cosine, sine = atom_group(
                lay, atoms_ref, waves_ref, group, True
            )
            third = wave_rows(cosine, sine, cos_ref, sin_ref, row_of(kinds[0], 2))
            third_slope = wave_rows(cosine, sine, cos_ref, sin_ref, row_of(kinds[1], 2))
            starts = [starts_ref[base + block] for block in range(lay.pack)]
            weights, weight_slopes = line_weights(cells, kinds, starts)
            rights = []
            for block in range(lay.pack):
                both = jnp.concatenate([entry[:, lanes_of(block)] for entry in wide], axis=1)
                high, low = halves_of(both)
                rights.append((jnp.concatenate([high, high], axis=0), low))

            def found_at(line, block):
                where = rows_at(lay, line)
                field_high = high_ref[0, where, :]
                field = jnp.concatenate([field_high, low_ref[0, where, :]], axis=1)
                right, low = rights[block]
                return dot(field, right) + dot(field_high, low)

            def sums_of(found, weights, weight_slopes):
                plain = sloped = across = jnp.zeros((lay.wave_rows, LANES), jnp.float32)
                for i in range(CHUNK):
                    lines = slice(i * lay.wave_rows, (i + 1) * lay.wave_rows)
                    value = found[lines, :LANES]
                    plain += value * weights[i : i + 1]
                    across += value * weight_slopes[i : i + 1]
                    sloped += found[lines, LANES:] * weights[i : i + 1]
                return sloped, across, plain

            founds = [found_at(starts[block], block) for block in range(lay.pack)]
            for block in range(lay.pack):
                lanes = lanes_of(block)
                sums = sums_of(founds[block], weights[:, lanes], weight_slopes[:, lanes])
                factors = (third[:, lanes], third[:, lanes], third_slope[:, lanes])
                for dimension in range(3):
                    total = jnp.sum(sums[dimension] * factors[dimension], axis=0, keepdims=True)
                    out_ref[0, 0, dimension, pl.ds(first + block, 1), :] = -charge[:, lanes] * total
            for block in range(lay.pack):

                @pl.loop(1, turns_ref[base + block])
                def more(turn):
                    line = starts[block] + turn * CHUNK
                    lanes = lanes_of(block)
                    more_weights, more_slopes = line_weights(
                        cells[:, lanes], pick(kinds, block), [line]
                    )
                    sums = sums_of(found_at(line, block), more_weights, more_slopes)
                    factors = (third[:, lanes], third[:, lanes], third_slope[:, lanes])
                    for dimension in range(3):
                        total = jnp.sum(sums[dimension] * factors[dimension], axis=0, keepdims=True)
                        out_ref[0, 0, dimension, pl.ds(first + block, 1), :] += (
                            -charge[:, lanes] * total
                        )


def sample(lay, starts, turns, atoms, waves, cosines, sines, high, low):
    size = lay.lines_padded * lay.wave_rows
    field = pl.BlockSpec((1, size, LANES), lambda row, part, *refs: (row, 0, 0))
    shape = (lay.rows, lay.half_cols, 3, lay.blocks, LANES)
    return pl.pallas_call(
        functools.partial(sample_kernel, lay),
        grid_spec=pltpu.PrefetchScalarGridSpec(
            num_scalar_prefetch=2,
            grid=(lay.rows, lay.half_cols),
            in_specs=atom_specs(lay) + [field, field],
            out_specs=pl.BlockSpec((1, 1) + shape[2:], lambda row, part, *refs: (row, part, 0, 0, 0)),
        ),
        out_shape=jax.ShapeDtypeStruct(shape, jnp.float32),
        compiler_params=pltpu.CompilerParams(vmem_limit_bytes=40 * 1024 * 1024),
        cost_estimate=pl.CostEstimate(flops=10**10, bytes_accessed=10**7, transcendentals=0),
        name="sample",
    )(starts, turns, atoms, waves, cosines, sines, high, low)


def transform_kernel(
    lay,
    mesh_ref,
    *refs,
):
    message_refs = refs[: lay.rows]
    (
        first_high,
        first_low,
        second_high,
        second_low,
        back_high,
        back_low,
        last_high,
        last_low,
        out_high,
        out_low,
        field_ref,
        mine_ref,
        send_ref,
        recv_ref,
        home_ref,
        extra_ref,
        green_ref,
        send_sem,
        recv_sem,
        back_sem,
        home_sem,
        green_sem,
    ) = refs[lay.rows :]
    row = lax.axis_index("row")
    col = lax.axis_index("col")
    side = col % 2
    partner = (row, col + 1 - 2 * side)
    lines, length, own, padded = lay.lines, lay.length, lay.own, lay.slots_padded
    inner = lines - HALO

    number = message_number(lay, row, col)

    def green_copy(index):
        spot = lax.rem(index - number + lay.rows, lay.rows)
        return pltpu.make_async_copy(message_refs[index], green_ref.at[spot], green_sem.at[index])

    for index in range(lay.rows):
        green_copy(index).start()

    def three(high, low, table_high, table_low):
        return dot(high, table_high) + dot(low, table_high) + dot(high, table_low)

    def push(index):
        return pltpu.make_async_remote_copy(
            src_ref=send_ref.at[index],
            dst_ref=recv_ref.at[index],
            send_sem=send_sem.at[index],
            recv_sem=recv_sem.at[index],
            device_id=partner,
            device_id_type=MESH,
        )

    def push_back(index):
        return pltpu.make_async_remote_copy(
            src_ref=send_ref.at[index],
            dst_ref=home_ref.at[index],
            send_sem=back_sem.at[index],
            recv_sem=home_sem.at[index],
            device_id=partner,
            device_id_type=MESH,
        )

    def forward(slot):
        rows = [
            jnp.concatenate(
                [mesh_ref[r, pl.ds(start, lines, stride=lay.stride), :] for r in range(lay.rows)],
                axis=1,
            )
            for start in (slot, padded + slot)
        ]
        high, low = halves_of(jnp.concatenate(rows, axis=0))
        found = three(high, low, first_high[...], first_low[...])
        upper, lower = found[:lines], found[lines:]
        return upper[:, :length], upper[:, length:], lower[:, :length], lower[:, length:]

    for base, target in ((0, send_ref), (own, mine_ref)):
        away = base == 0

        @pl.loop(0, own)
        def first_pass(i):
            real_cos, real_sin, imag_cos, imag_sin = forward(base + i)

            @pl.when(i == 0)
            def mirrored():
                target[own, 0] = real_cos - imag_sin
                target[own, 1] = -imag_cos - real_sin

            target[i, 0] = real_cos + imag_sin
            target[i, 1] = imag_cos - real_sin
            if away:

                @pl.when(i == 0)
                def start_mirrored():
                    push(own).start()

                push(i).start()

    @pl.loop(0, own + 1)
    def sent(i):
        push(i).wait_send()

    for index in range(lay.rows):
        green_copy(index).wait()

    def spectrum(index):
        mine, other = mine_ref[index], recv_ref[index]
        parts = []
        for part in range(2):
            a, b = mine[part], other[part]
            parts.append(
                jnp.concatenate(
                    [
                        a[HALO:inner],
                        a[inner:] + b[:HALO],
                        b[HALO:inner],
                        b[inner:] + a[:HALO],
                    ],
                    axis=0,
                )
            )
        high, low = halves_of(jnp.concatenate(parts, axis=1))
        found = (
            dot(second_high[...], high) + dot(second_high[...], low) + dot(second_low[...], high)
        )
        cos_part, sin_part = found[:length], found[length:]
        real = cos_part[:, :length] + sin_part[:, length:]
        imag = cos_part[:, length:] - sin_part[:, :length]
        blocks = [green_ref[r, index] for r in range(lay.rows)]
        green = jnp.concatenate(blocks, axis=0)
        return real * green, imag * green

    push(own).wait_recv()
    extra_ref[0], extra_ref[1] = spectrum(own)

    @pl.loop(0, own)
    def second_pass(i):
        push(i).wait_recv()
        real, imag = spectrum(i)
        first = jnp.where(i == 0, 1.0, 0.0)
        real += first * extra_ref[0]
        imag += first * extra_ref[1]
        high, low = halves_of(jnp.concatenate([real, imag], axis=1))
        found = dot(back_high[...], high) + dot(back_high[...], low) + dot(back_low[...], high)
        cos_part, sin_part = found[: 2 * lines], found[2 * lines :]
        real = cos_part[:, :length] - sin_part[:, length:]
        imag = cos_part[:, length:] + sin_part[:, :length]
        mine_ref[i, 0] = real[:lines]
        mine_ref[i, 1] = imag[:lines]
        send_ref[i, 0] = real[lines:]
        send_ref[i, 1] = imag[lines:]
        push_back(i).start()

    cleared = 0 if lay.slots < padded else lines * lay.stride // 8 * 8
    total_rows = mesh_ref.shape[1]
    for r in range(lay.rows):
        field_ref[r, pl.ds(cleared, total_rows - cleared), :] = jnp.zeros(
            (total_rows - cleared, LANES), jnp.float32
        )

    def last(local, planes_ref, i):
        high, low = halves_of(jnp.concatenate([planes_ref[i, 0], planes_ref[i, 1]], axis=1))
        found = three(high, low, last_high[...], last_low[...])
        for part in range(2):
            for r in range(lay.rows):
                lanes = (part * lay.rows + r) * LANES
                where = pl.ds(part * padded + local, lines, stride=lay.stride)
                field_ref[r, where, :] = found[:, lanes : lanes + LANES]

    @pl.loop(0, own)
    def last_mine(i):
        last(own + i, mine_ref, i)

    @pl.loop(0, own)
    def last_home(i):
        push_back(i).wait_recv()
        last(i, home_ref, i)

    @pl.loop(0, lay.lines_padded)
    def split(line):
        where = pl.ds(pl.multiple_of(line * lay.wave_rows, lay.wave_rows), lay.wave_rows)
        for r in range(lay.rows):
            value = field_ref[r, pl.ds(line * lay.stride, lay.wave_rows), :]
            out_high[r, where, :], out_low[r, where, :] = halves_of(value)

    @pl.loop(0, own)
    def returned(i):
        push_back(i).wait_send()


def message_number(lay, row, col):
    member = lax.rem(row, lay.group)
    frame = row // lay.group
    return (lax.rem(col, 2) * lay.frames + frame) * lay.splits + lax.rem(member, lay.splits)


def transform(lay, mesh, messages, tables):
    dma = pltpu.SemaphoreType.DMA
    plane = (2, lay.lines, lay.length)
    vmem = pl.BlockSpec(memory_space=pltpu.VMEM)
    out = jax.ShapeDtypeStruct(
        (lay.rows, lay.lines_padded * lay.wave_rows, LANES), jnp.bfloat16
    )
    return pl.pallas_call(
        functools.partial(transform_kernel, lay),
        in_specs=[vmem] + [pl.BlockSpec(memory_space=pl.ANY)] * lay.rows + [vmem] * len(tables),
        out_specs=[vmem, vmem],
        out_shape=[out, out],
        scratch_shapes=[
            pltpu.VMEM(mesh.shape, jnp.float32),
            pltpu.VMEM((lay.own + 1,) + plane, jnp.float32),
            pltpu.VMEM((lay.own + 1,) + plane, jnp.float32),
            pltpu.VMEM((lay.own + 1,) + plane, jnp.float32),
            pltpu.VMEM((lay.own,) + plane, jnp.float32),
            pltpu.VMEM((2, lay.length, lay.length), jnp.float32),
            pltpu.VMEM((lay.rows,) + messages[0].shape, jnp.float32),
            dma((lay.own + 1,)),
            dma((lay.own + 1,)),
            dma((lay.own,)),
            dma((lay.own,)),
            dma((lay.rows,)),
        ],
        compiler_params=pltpu.CompilerParams(
            has_side_effects=True, vmem_limit_bytes=62 * 1024 * 1024
        ),
        cost_estimate=pl.CostEstimate(flops=10**10, bytes_accessed=10**7, transcendentals=0),
        name="transform",
    )(mesh, *messages, *tables)


def table_halves(value):
    leading = lax.reduce_precision(value, exponent_bits=8, mantissa_bits=7)
    return leading.astype(jnp.bfloat16), (value - leading).astype(jnp.bfloat16)


def make_tables(lay, side):
    length, half = lay.length, lay.half_cols * lay.block_cols
    waves = jnp.arange(length, dtype=jnp.int32)
    spots = jnp.arange(LANES, dtype=jnp.int32)
    blocks = jnp.arange(lay.rows, dtype=jnp.int32)
    zero = lax.optimization_barrier(jnp.int32(0))
    across = (blocks[:, None] * lay.block_rows + spots[None, :] - HALO).reshape(-1) + length + zero
    valid = jnp.tile(spots < lay.span, lay.rows)
    cosine, sine = phases(across[:, None] * waves[None, :], length)
    keep = valid[:, None]
    first = jnp.where(keep, jnp.concatenate([cosine, sine], axis=1), 0.0)
    cosine, sine = phases(across[None, :] * waves[:, None], length)
    top = jnp.concatenate([cosine, sine], axis=1)
    bottom = jnp.concatenate([-sine, cosine], axis=1)
    last = jnp.where(jnp.tile(valid, 2)[None, :], jnp.concatenate([top, bottom], axis=0), 0.0)
    along = waves + half * side
    second = jnp.concatenate(phases(waves[:, None] * along[None, :], length), axis=0)
    near = jnp.arange(lay.lines, dtype=jnp.int32) - HALO + length
    both = jnp.concatenate([near + half * side, near + half * (1 - side)])
    back = jnp.concatenate(phases(both[:, None] * waves[None, :], length), axis=0)
    tables = []
    for table in (first, second, back, last):
        tables.extend(table_halves(table))
    return tables


def make_waves(lay, row, col, side):
    length = lay.length
    member = row % lay.group
    source = 2 * (col // 2) + member // lay.splits
    split = member % lay.splits
    start = lay.block_cols * source + jnp.where(source >= lay.half_cols, 1, 0) + split * lay.slots
    index = jnp.arange(lay.slots_padded, dtype=jnp.int32)
    slot = jnp.where(index < lay.own, (1 - side) * lay.own, side * lay.own) + index % lay.own
    special = (source == 0) & (split == 0) & (slot == 0)
    waves = jnp.concatenate([start + slot, jnp.where(special, length // 2, start + slot)])
    turns = jnp.concatenate([jnp.zeros_like(slot), jnp.where(special, 0, length // 4)])
    live = jnp.tile(index < lay.slots, 2)[None, :, None]
    offsets = jnp.arange(6, dtype=jnp.int32)
    cosine, sine = phases(offsets[:, None] * waves[None, :], length)
    shape = (6, lay.wave_rows, LANES)
    cosines = jnp.broadcast_to(jnp.where(live, cosine[:, :, None], 0.0), shape)
    sines = jnp.broadcast_to(jnp.where(live, sine[:, :, None], 0.0), shape)
    both = jnp.broadcast_to(jnp.stack([waves, turns])[:, :, None], (2, lay.wave_rows, LANES))
    return both, cosines, sines


def share_green(lay, influence, row, col):
    length = lay.length
    rows, cols = lay.rows, lay.cols
    scale = 1.0 / float(length) ** 3
    used = lay.block_cols // 2
    offset = jnp.where(col >= lay.half_cols, 1, 0)
    middle = lax.ppermute(influence[:, 0, :], "col", [(lay.half_cols, 0)])
    block = lax.dynamic_slice_in_dim(influence, offset, used, axis=1).transpose(1, 0, 2)
    block = block.reshape(lay.splits, 2, lay.own, lay.block_rows, length)
    special = col == 0
    zeroth = block[0, 0, 0]
    extra = jnp.where(special, (0.5 * scale) * (zeroth - middle), 0.0)
    zeroth = jnp.where(special, (0.5 * scale) * (zeroth + middle), (2.0 * scale) * zeroth)
    block = jnp.concatenate([(2.0 * scale) * block, jnp.zeros_like(block[:, :, :1])], axis=2)
    block = block.at[0, 0, 0].set(zeroth).at[0, 0, lay.own].set(extra)
    block = block.reshape((2 * lay.splits,) + block.shape[2:])
    messages = []
    for number in range(rows):
        message = (number - row) % rows
        split = message % lay.splits
        side = message // (lay.frames * lay.splits)
        sent = lax.dynamic_index_in_dim(block, split * 2 + side, keepdims=False)
        pairs = []
        for r in range(rows):
            at = (number - r) % rows
            to_split, rest = at % lay.splits, at // lay.splits
            to_frame, to_side = rest % lay.frames, rest // lay.frames
            for c in range(cols):
                to_row = to_frame * lay.group + (c % 2) * lay.splits + to_split
                pairs.append((r * cols + c, to_row * cols + 2 * (c // 2) + to_side))
        messages.append(lax.ppermute(sent, ("row", "col"), pairs))
    return messages


def forces_of(cell_index, fraction, charge, atom_count, influence):
    frames, _, atoms = fraction.shape
    lay = Layout(frames, influence.shape[2], atoms)
    row = lax.axis_index("row")
    col = lax.axis_index("col")
    side = col % 2
    messages = share_green(lay, influence, row, col)
    tables = make_tables(lay, side)
    waves, cosines, sines = make_waves(lay, row, col, side)

    slot_ids = jnp.arange(atoms, dtype=jnp.int32)
    alive = slot_ids[None, :] < atom_count
    charges = jnp.where(alive, charge, 0.0)
    origin = jnp.stack([row * lay.block_rows, (col // lay.half_cols) * lay.half_cols * lay.block_cols, 0])
    cells = cell_index - origin[None, :, None]
    payload = jnp.concatenate(
        [
            cells.astype(jnp.float32),
            fraction,
            charges[:, None, :],
            alive[:, None, :].astype(jnp.float32),
        ],
        axis=1,
    )
    key = (jnp.where(alive, cells[:, 1], lay.length) * atoms + slot_ids[None, :]).astype(jnp.float32)
    key_col = jnp.broadcast_to(key[:, :, None], (frames, atoms, LANES))
    sorted_atoms, rank = sort_atoms(key[:, None, :], key_col, payload)
    shared = gather_atoms(lay, sorted_atoms)

    lines = shared[:, :, 1, :].reshape(lay.rows * lay.half_cols * lay.blocks, LANES)
    lives = shared[:, :, 7, :].reshape(lines.shape) > 0.5
    lowest = jnp.min(jnp.where(lives, lines, 1024.0), axis=1).astype(jnp.int32)
    highest = jnp.max(jnp.where(lives, lines, -1024.0), axis=1).astype(jnp.int32)
    live = highest >= lowest
    starts = jnp.where(live, lowest + HALO - 5, 0)
    turns = jnp.where(live, (highest - lowest + 6 + CHUNK - 1) // CHUNK, 0)

    mesh = spread(lay, starts, turns, shared, waves, cosines, sines)
    high, low = transform(lay, mesh, messages, tables)
    partial = sample(lay, starts, turns, shared, waves, cosines, sines, high, low)
    returned = return_forces(lay, partial)
    forces = jnp.sum(returned, axis=1).reshape(frames, 3, atoms)
    forces = jnp.pad(forces, ((0, 0), (0, 5), (0, 0)))
    return unsort_forces(rank, forces)[:, :3]


def solution(mesh):
    placed = (
        P(None, None, ("row", "col")),
        P(None, None, ("row", "col")),
        P(None, ("row", "col")),
        P(None, ("row", "col")),
        P("row", "col", None),
    )
    return jax.shard_map(
        forces_of, mesh=mesh, in_specs=placed, out_specs=P(None, None, ("row", "col")), check_vma=False
    )
```

```python
import functools
import math

import jax
import jax.numpy as jnp
import numpy as np
from jax import lax
from jax.experimental import pallas as pl
from jax.experimental.pallas import tpu as pltpu
from jax.sharding import PartitionSpec as P


MESH = pl.DeviceIdType.MESH
LANES = 128
CHUNK = 10
PACK = 4
HALO = 8
NT = (((1,), (1,)), ((), ()))
NN = (((1,), (0,)), ((), ()))


def dot(left, right, form=NN):
    return lax.dot_general(left, right, form, preferred_element_type=jnp.float32)


def halves_of(value):
    high = value.astype(jnp.bfloat16)
    return high, (value - high.astype(jnp.float32)).astype(jnp.bfloat16)


def spline_rows(fraction):
    nothing = jnp.zeros_like(fraction)
    levels = [fraction, 1.0 - fraction]
    slopes = levels
    for degree in range(3, 7):
        padded = levels + [nothing]
        following = []
        for offset in range(degree):
            beneath = padded[offset - 1] if offset > 0 else nothing
            following.append(
                ((fraction + offset) * padded[offset] + (degree - fraction - offset) * beneath)
                * (1.0 / (degree - 1))
            )
        if degree == 6:
            slopes = [
                padded[offset] - (padded[offset - 1] if offset > 0 else nothing)
                for offset in range(6)
            ]
        levels = following
    return levels, slopes


def dense(distance, lists):
    results = [jnp.zeros(distance.shape, jnp.float32) for _ in lists]
    for offset in range(6):
        hit = distance == offset
        results = [jnp.where(hit, rows[offset], result) for rows, result in zip(lists, results)]
    return results


def row_of(lists, dimension):
    starts = range(dimension, lists[0].shape[0], 3)
    return [
        jnp.concatenate([entry[start : start + 1, :] for start in starts], axis=1)
        for entry in lists
    ]


def phases(product, length):
    half = length // 2
    moved = product + half
    if length & (length - 1):
        turned = lax.rem(moved, length) - half
    else:
        turned = (moved & (length - 1)) - half
    angle = turned.astype(jnp.float32) * (2.0 * math.pi / length / 4.0)
    square = angle * angle
    sine = angle * (
        1.0
        + square
        * (-1.0 / 6 + square * (1.0 / 120 + square * (-1.0 / 5040 + square * (1.0 / 362880))))
    )
    cosine = 1.0 + square * (
        -0.5
        + square
        * (1.0 / 24 + square * (-1.0 / 720 + square * (1.0 / 40320 - square * (1.0 / 3628800))))
    )
    for _ in range(2):
        sine, cosine = 2.0 * sine * cosine, 1.0 - 2.0 * sine * sine
    return cosine, sine


def wave_rows(cosine, sine, cos_ref, sin_ref, packed_ref, cells, rows):
    copies = cosine.shape[1] // LANES

    def wide(ref, offset):
        return jnp.concatenate([ref[offset]] * copies, axis=1) * rows[offset]

    even, odd = wide(cos_ref, 0), wide(sin_ref, 0)
    for offset in range(1, 6):
        even += wide(cos_ref, offset)
        odd += wide(sin_ref, offset)
    real = cosine * even + sine * odd
    imag = cosine * odd - sine * even
    middle = rows[0] - rows[1] + rows[2] - rows[3] + rows[4] - rows[5]
    middle = jnp.where((cells & 1) == 0, middle, -middle)
    packed = jnp.concatenate([packed_ref[...]] * copies, axis=1)
    return jnp.concatenate([real, jnp.where(packed > 0.5, middle, imag)], axis=0)


def sort_kernel(bins, width, payload_ref, sorted_ref, rank_ref):
    atoms = payload_ref.shape[2]
    blocks = atoms // LANES
    line = payload_ref[0, 1:2, :]
    line = line - width * jnp.floor((line + 0.5) * (1.0 / width))
    line = jnp.where(payload_ref[0, 7:8, :] > 0.5, line.astype(jnp.int32), bins - 1)
    kinds = lax.broadcasted_iota(jnp.int32, (bins, LANES), 0)
    marks = [jnp.where(line[:, lanes_of(block)] == kinds, 1.0, 0.0) for block in range(blocks)]
    across = lax.broadcasted_iota(jnp.int32, (LANES, LANES), 0)
    down = lax.broadcasted_iota(jnp.int32, (LANES, LANES), 1)
    before = jnp.where(across < down, 1.0, 0.0).astype(jnp.bfloat16)
    every = jnp.ones((LANES, LANES), jnp.bfloat16)
    packed = jnp.concatenate(marks, axis=0).astype(jnp.bfloat16)
    earlier = dot(packed, before)
    counts = dot(packed, every)
    running = jnp.zeros((bins, LANES), jnp.float32)
    partial = []
    for block in range(blocks):
        partial.append(running + earlier[block * bins : (block + 1) * bins])
        running += counts[block * bins : (block + 1) * bins]
    lower = lax.broadcasted_iota(jnp.int32, (bins, bins), 1) < lax.broadcasted_iota(
        jnp.int32, (bins, bins), 0
    )
    lower = jnp.where(lower, 1.0, 0.0).astype(jnp.bfloat16)
    high, low = halves_of(running)
    base = dot(lower, high) + dot(lower, low)
    for block in range(blocks):
        places = marks[block] * (partial[block] + base)
        rank_ref[0, :, block * LANES : (block + 1) * LANES] = jnp.sum(places, axis=0, keepdims=True)

    value = payload_ref[0]
    first, rest = halves_of(value)
    left = value - first.astype(jnp.float32)
    third = (left - rest.astype(jnp.float32)).astype(jnp.bfloat16)
    pieces = jnp.concatenate([first, rest, third, jnp.zeros_like(first)], axis=0)
    rank = rank_ref[0].astype(jnp.int32)
    size = math.gcd(256, atoms)

    @pl.loop(0, atoms // size)
    def place(part):
        start = pl.multiple_of(part * size, size)
        spots = lax.broadcasted_iota(jnp.int32, (size, atoms), 0) + start
        chosen = jnp.where(rank == spots, 1.0, 0.0).astype(jnp.bfloat16)
        moved = dot(pieces, chosen, NT)
        sorted_ref[0, :, pl.ds(start, size)] = moved[0:8] + moved[8:16] + moved[16:24]


def sort_atoms(lay, payload):
    frames, rows, atoms = payload.shape
    whole = lambda frame: (frame, 0, 0)
    bins = -(-(lay.block_cols + 1) // 16) * 16
    return pl.pallas_call(
        functools.partial(sort_kernel, bins, lay.block_cols),
        grid=(frames,),
        in_specs=[pl.BlockSpec((1, rows, atoms), whole)],
        out_specs=[pl.BlockSpec((1, rows, atoms), whole), pl.BlockSpec((1, 1, atoms), whole)],
        out_shape=[
            jax.ShapeDtypeStruct((frames, rows, atoms), jnp.float32),
            jax.ShapeDtypeStruct((frames, 1, atoms), jnp.float32),
        ],
        compiler_params=pltpu.CompilerParams(vmem_limit_bytes=32 * 1024 * 1024),
        name="sort_atoms",
    )(payload)


def unsort_kernel(rank_ref, force_ref, out_ref):
    atoms = rank_ref.shape[2]
    value = force_ref[0]
    high, low = halves_of(value)
    left = value - high.astype(jnp.float32)
    third = (left - low.astype(jnp.float32)).astype(jnp.bfloat16)
    pieces = jnp.concatenate([high, low, third, jnp.zeros_like(high)], axis=0)
    rank = rank_ref[0].astype(jnp.int32)
    width = math.gcd(256, atoms)

    @pl.loop(0, atoms // width)
    def place(part):
        start = pl.multiple_of(part * width, width)
        spots = lax.broadcasted_iota(jnp.int32, (atoms, width), 0)
        lanes = pl.ds(start, width)
        here = rank_ref[0, :, lanes].astype(jnp.int32)
        chosen = jnp.where(here == spots, 1.0, 0.0).astype(jnp.bfloat16)
        moved = dot(pieces, chosen, NN)
        out_ref[0, :, lanes] = moved[0:8] + moved[8:16] + moved[16:24]


def unsort_forces(rank, forces):
    frames, rows, atoms = forces.shape
    whole = lambda frame: (frame, 0, 0)
    return pl.pallas_call(
        unsort_kernel,
        grid=(frames,),
        in_specs=[pl.BlockSpec((1, 1, atoms), whole), pl.BlockSpec((1, rows, atoms), whole)],
        out_specs=pl.BlockSpec((1, rows, atoms), whole),
        out_shape=jax.ShapeDtypeStruct((frames, rows, atoms), jnp.float32),
        compiler_params=pltpu.CompilerParams(vmem_limit_bytes=32 * 1024 * 1024),
        name="unsort_forces",
    )(rank, forces)


class Layout:
    def __init__(self, frames, length, atoms):
        self.rows = lax.axis_size("row")
        self.cols = lax.axis_size("col")
        self.frames = frames
        self.length = length
        self.atoms = atoms
        self.group = self.rows // frames
        self.half_cols = self.cols // 2
        self.block_rows = length // self.rows
        self.block_cols = length // self.cols
        self.slots = length // 2 // (self.group * self.half_cols)
        self.own = self.slots // 2
        self.slots_padded = max(8, self.slots)
        self.wave_rows = 2 * self.slots_padded
        self.stride = self.wave_rows + 1
        self.lines = self.half_cols * self.block_cols + HALO
        self.lines_padded = -(-(self.lines + CHUNK - 1) // 8) * 8
        self.splits = self.group // 2
        self.blocks = atoms // LANES
        self.span = self.block_rows + HALO
        self.pack = math.gcd(PACK, self.blocks)


def gather_kernel(lay, mine_ref, all_ref, local_sem, send_sem, recv_sem, pass_sem, took_sem):
    row = lax.axis_index("row")
    col = lax.axis_index("col")
    pair = col // 2
    side = col % 2
    half = col // lay.half_cols
    place = col % lay.half_cols
    hub = half == side
    pair_start = (2 * pair) % lay.half_cols

    def nearest(step):
        other = lax.rem(row // lay.group + step // lay.group, lay.frames)
        return other * lay.group + lax.rem(row + step, lay.group)

    def first_send(frame, member):
        target = frame * lay.group + member
        index = frame * lay.group + member
        return target, pltpu.make_async_remote_copy(
            src_ref=mine_ref.at[frame],
            dst_ref=all_ref.at[row, place],
            send_sem=send_sem.at[index],
            recv_sem=recv_sem.at[row, side],
            device_id=(target, 2 * pair + half),
            device_id_type=MESH,
        )

    def self_copy(frame):
        return pltpu.make_async_copy(mine_ref.at[frame], all_ref.at[row, place], local_sem)

    for frame in range(lay.frames):
        for member in range(lay.group):
            target, copy = first_send(frame, member)
            alone = (target == row) & hub

            @pl.when(jnp.logical_not(alone))
            def send():
                copy.start()

            @pl.when(alone)
            def keep():
                self_copy(frame).start()

    def second_send(source, part, other):
        spot = pair_start + part
        return pltpu.make_async_remote_copy(
            src_ref=all_ref.at[source, spot],
            dst_ref=all_ref.at[source, spot],
            send_sem=pass_sem.at[source, part, other - 1],
            recv_sem=took_sem.at[source, spot],
            device_id=(row, 2 * ((pair + other) % lay.half_cols) + side),
            device_id_type=MESH,
        )

    def arrival(source, spot, sem):
        return pltpu.make_async_remote_copy(
            src_ref=all_ref.at[source, spot],
            dst_ref=all_ref.at[source, spot],
            send_sem=send_sem.at[0],
            recv_sem=sem,
            device_id=(row, col),
            device_id_type=MESH,
        )

    @pl.when(hub)
    def forward():
        for step in range(lay.rows):
            source = nearest(step)
            for part in range(2):
                spot = pair_start + part
                alone = (source == row) & (part == side)

                @pl.when(jnp.logical_not(alone))
                def landed():
                    arrival(source, spot, recv_sem.at[source, part]).wait_recv()

                @pl.when(alone)
                def kept():
                    self_copy(row // lay.group).wait()

                for other in range(1, lay.half_cols):
                    second_send(source, part, other).start()

    for frame in range(lay.frames):
        for member in range(lay.group):
            target, copy = first_send(frame, member)

            @pl.when(jnp.logical_not((target == row) & hub))
            def sent():
                copy.wait_send()

    for spot in range(lay.half_cols):
        local = hub & (pair == side * (lay.half_cols // 2) + spot // 2)

        @pl.when(jnp.logical_not(local))
        def took():
            for source in range(lay.rows):
                arrival(source, spot, took_sem.at[source, spot]).wait_recv()

    @pl.when(hub)
    def passed():
        for source in range(lay.rows):
            for part in range(2):
                for other in range(1, lay.half_cols):
                    second_send(source, part, other).wait_send()


def gather_atoms(lay, mine):
    _, rows, atoms = mine.shape
    dma = pltpu.SemaphoreType.DMA
    return pl.pallas_call(
        functools.partial(gather_kernel, lay),
        in_specs=[pl.BlockSpec(memory_space=pltpu.VMEM)],
        out_specs=pl.BlockSpec(memory_space=pltpu.VMEM),
        out_shape=jax.ShapeDtypeStruct((lay.rows, lay.half_cols, rows, atoms), jnp.float32),
        scratch_shapes=[
            dma,
            dma((lay.rows,)),
            dma((lay.rows, 2)),
            dma((lay.rows, 2, lay.half_cols - 1)),
            dma((lay.rows, lay.half_cols)),
        ],
        compiler_params=pltpu.CompilerParams(has_side_effects=True),
        name="gather_atoms",
    )(mine)


def return_kernel(lay, force_ref, out_ref, local_sem, send_sem, recv_sem):
    row = lax.axis_index("row")
    col = lax.axis_index("col")
    side = col % 2
    frame = row // lay.group
    index = (row % lay.group) * lay.half_cols + col // 2
    copies = []
    for source in range(lay.rows):
        for spot in range(lay.half_cols):
            owner = side * lay.half_cols + spot
            copies.append(
                (
                    (source == row) & (owner == col),
                    pltpu.make_async_remote_copy(
                        src_ref=force_ref.at[source, spot],
                        dst_ref=out_ref.at[frame, index],
                        send_sem=send_sem.at[source, spot],
                        recv_sem=recv_sem.at[frame, index],
                        device_id=(source, owner),
                        device_id_type=MESH,
                    ),
                    pltpu.make_async_copy(
                        force_ref.at[source, spot], out_ref.at[frame, index], local_sem
                    ),
                )
            )
    for alone, copy, local in copies:

        @pl.when(jnp.logical_not(alone))
        def send():
            copy.start()

        @pl.when(alone)
        def keep():
            local.start()

    for alone, copy, local in copies:

        @pl.when(jnp.logical_not(alone))
        def sent():
            copy.wait_send()

        @pl.when(alone)
        def kept():
            local.wait()

    half = col // lay.half_cols
    for from_frame in range(lay.frames):
        for member in range(lay.group):
            for pair in range(lay.half_cols):
                slot = member * lay.half_cols + pair
                alone = (from_frame * lay.group + member == row) & (2 * pair + half == col)

                @pl.when(jnp.logical_not(alone))
                def landed():
                    pltpu.make_async_remote_copy(
                        src_ref=out_ref.at[from_frame, slot],
                        dst_ref=out_ref.at[from_frame, slot],
                        send_sem=send_sem.at[0, 0],
                        recv_sem=recv_sem.at[from_frame, slot],
                        device_id=(row, col),
                        device_id_type=MESH,
                    ).wait_recv()


def return_forces(lay, forces):
    rows, half_cols = forces.shape[:2]
    members = lay.group * half_cols
    dma = pltpu.SemaphoreType.DMA
    return pl.pallas_call(
        functools.partial(return_kernel, lay),
        in_specs=[pl.BlockSpec(memory_space=pltpu.VMEM)],
        out_specs=pl.BlockSpec(memory_space=pltpu.VMEM),
        out_shape=jax.ShapeDtypeStruct((lay.frames, members) + forces.shape[2:], jnp.float32),
        scratch_shapes=[dma, dma((rows, half_cols)), dma((lay.frames, members))],
        compiler_params=pltpu.CompilerParams(has_side_effects=True),
        name="return_forces",
    )(forces)


def atom_group(lay, atoms_ref, waves_ref, group, with_slopes):
    width = lay.pack * LANES
    lanes = pl.ds(pl.multiple_of(group * width, width), width)
    piece = atoms_ref[0, 0, :, lanes]
    cells = piece[0:3].astype(jnp.int32)
    packed = [piece[3:6, lanes_of(block)] for block in range(lay.pack)]
    values, slopes = spline_rows(jnp.concatenate(packed, axis=0))
    charge = piece[6:7]
    spots = lax.broadcasted_iota(jnp.int32, (lay.span, width), 0)
    kinds = [values, slopes] if with_slopes else [values]
    wide = dense(cells[0:1] + HALO - spots, [row_of(kind, 0) for kind in kinds])
    pad = jnp.zeros((LANES - lay.span, width), jnp.float32)
    wide = [jnp.concatenate([entry, pad], axis=0) for entry in wide]
    turned = jnp.concatenate([waves_ref[...]] * lay.pack, axis=1) * cells[2:3]
    cosine, sine = phases(turned, lay.length)
    return cells, kinds, charge, wide, cosine, sine


def line_weights(cells, kinds, starts):
    lines = lax.broadcasted_iota(jnp.int32, (-(-CHUNK // 8) * 8, LANES), 0)
    lines = jnp.concatenate([lines + start for start in starts], axis=1)
    return dense(cells[1:2] + HALO - lines, [row_of(kind, 1) for kind in kinds])


def lanes_of(block):
    return slice(block * LANES, (block + 1) * LANES)


def pick(kinds, block):
    return [[row[3 * block : 3 * block + 3] for row in kind] for kind in kinds]


def rows_at(lay, line):
    return pl.ds(pl.multiple_of(line * lay.wave_rows, lay.wave_rows), CHUNK * lay.wave_rows)


def spread_kernel(
    lay, starts_ref, turns_ref, atoms_ref, waves_ref, packed_ref, cos_ref, sin_ref, mesh_ref
):
    part = pl.program_id(1)
    pencil = pl.program_id(0) * lay.half_cols + part

    @pl.when(part == 0)
    def clear():
        mesh_ref[...] = jnp.zeros_like(mesh_ref)

    @pl.loop(0, lay.blocks // lay.pack)
    def add_group(group):
        base = pencil * lay.blocks + group * lay.pack

        @pl.when(turns_ref[base] > 0)
        def live():
            cells, kinds, charge, wide, cosine, sine = atom_group(
                lay, atoms_ref, waves_ref, group, False
            )
            tables = cosine, sine, cos_ref, sin_ref, packed_ref
            waves = wave_rows(*tables, cells[2:3], row_of(kinds[0], 2)) * charge
            starts = [starts_ref[base + block] for block in range(lay.pack)]
            (weights,) = line_weights(cells, kinds, starts)
            rights = []
            for block in range(lay.pack):
                high, low = halves_of(wide[0][:, lanes_of(block)])
                rights.append(
                    jnp.concatenate(
                        [
                            jnp.concatenate([high, high], axis=1),
                            jnp.concatenate([low, low], axis=1),
                        ],
                        axis=0,
                    )
                )

            def total_of(weights, block):
                wave = waves[:, lanes_of(block)]
                product = jnp.concatenate([weights[i : i + 1] * wave for i in range(CHUNK)], axis=0)
                high, low = halves_of(product)
                total = dot(jnp.concatenate([high, low], axis=1), rights[block], NT)
                return total[:, :LANES] + total[:, LANES:]

            totals = [total_of(weights[:, lanes_of(block)], block) for block in range(lay.pack)]

            def add(line, total):
                for i in range(CHUNK):
                    part = total[i * lay.wave_rows : (i + 1) * lay.wave_rows]
                    mesh_ref[0, pl.ds((line + i) * lay.stride, lay.wave_rows), :] += part

            for block in range(lay.pack):
                add(starts[block], totals[block])
            for block in range(lay.pack):

                @pl.loop(1, turns_ref[base + block])
                def more(turn):
                    line = starts[block] + turn * CHUNK
                    lanes = lanes_of(block)
                    (weights,) = line_weights(cells[:, lanes], pick(kinds, block), [line])
                    add(line, total_of(weights, block))


def atom_specs(lay):
    fixed = lambda row, part, *refs: (0, 0, 0)
    return [
        pl.BlockSpec((1, 1, 8, lay.atoms), lambda row, part, *refs: (row, part, 0, 0)),
        pl.BlockSpec((lay.slots_padded, LANES), lambda row, part, *refs: (0, 0)),
        pl.BlockSpec((lay.slots_padded, LANES), lambda row, part, *refs: (0, 0)),
        pl.BlockSpec((6, lay.slots_padded, LANES), fixed),
        pl.BlockSpec((6, lay.slots_padded, LANES), fixed),
    ]


def spread(lay, starts, turns, atoms, waves):
    size = -(-lay.lines_padded * lay.stride // 8) * 8
    return pl.pallas_call(
        functools.partial(spread_kernel, lay),
        grid_spec=pltpu.PrefetchScalarGridSpec(
            num_scalar_prefetch=2,
            grid=(lay.rows, lay.half_cols),
            in_specs=atom_specs(lay),
            out_specs=pl.BlockSpec((1, size, LANES), lambda row, part, *refs: (row, 0, 0)),
        ),
        out_shape=jax.ShapeDtypeStruct((lay.rows, size, LANES), jnp.float32),
        compiler_params=pltpu.CompilerParams(vmem_limit_bytes=40 * 1024 * 1024),
        cost_estimate=pl.CostEstimate(flops=10**10, bytes_accessed=10**7, transcendentals=0),
        name="spread",
    )(starts, turns, atoms, *waves)


def sample_kernel(
    lay,
    starts_ref,
    turns_ref,
    atoms_ref,
    waves_ref,
    packed_ref,
    cos_ref,
    sin_ref,
    high_ref,
    low_ref,
    out_ref,
):
    pencil = pl.program_id(0) * lay.half_cols + pl.program_id(1)

    @pl.loop(0, lay.blocks // lay.pack)
    def sample_group(group):
        base = pencil * lay.blocks + group * lay.pack
        first = group * lay.pack

        @pl.when(turns_ref[base] == 0)
        def idle():
            for block in range(lay.pack):
                out_ref[0, 0, :, pl.ds(first + block, 1), :] = jnp.zeros((3, 1, LANES), jnp.float32)

        @pl.when(turns_ref[base] > 0)
        def live():
            cells, kinds, charge, wide, cosine, sine = atom_group(
                lay, atoms_ref, waves_ref, group, True
            )
            tables = cosine, sine, cos_ref, sin_ref, packed_ref
            third = wave_rows(*tables, cells[2:3], row_of(kinds[0], 2))
            third_slope = wave_rows(*tables, cells[2:3], row_of(kinds[1], 2))
            starts = [starts_ref[base + block] for block in range(lay.pack)]
            weights, weight_slopes = line_weights(cells, kinds, starts)
            rights = []
            for block in range(lay.pack):
                both = jnp.concatenate([entry[:, lanes_of(block)] for entry in wide], axis=1)
                high, low = halves_of(both)
                rights.append((jnp.concatenate([high, high], axis=0), low))

            def found_at(line, block):
                where = rows_at(lay, line)
                field_high = high_ref[0, where, :]
                field = jnp.concatenate([field_high, low_ref[0, where, :]], axis=1)
                right, low = rights[block]
                return dot(field, right) + dot(field_high, low)

            def sums_of(found, weights, weight_slopes):
                plain = sloped = across = jnp.zeros((lay.wave_rows, LANES), jnp.float32)
                for i in range(CHUNK):
                    lines = slice(i * lay.wave_rows, (i + 1) * lay.wave_rows)
                    value = found[lines, :LANES]
                    plain += value * weights[i : i + 1]
                    across += value * weight_slopes[i : i + 1]
                    sloped += found[lines, LANES:] * weights[i : i + 1]
                return sloped, across, plain

            founds = [found_at(starts[block], block) for block in range(lay.pack)]
            for block in range(lay.pack):
                lanes = lanes_of(block)
                sums = sums_of(founds[block], weights[:, lanes], weight_slopes[:, lanes])
                factors = (third[:, lanes], third[:, lanes], third_slope[:, lanes])
                for dimension in range(3):
                    total = jnp.sum(sums[dimension] * factors[dimension], axis=0, keepdims=True)
                    out_ref[0, 0, dimension, pl.ds(first + block, 1), :] = -charge[:, lanes] * total
            for block in range(lay.pack):

                @pl.loop(1, turns_ref[base + block])
                def more(turn):
                    line = starts[block] + turn * CHUNK
                    lanes = lanes_of(block)
                    more_weights, more_slopes = line_weights(
                        cells[:, lanes], pick(kinds, block), [line]
                    )
                    sums = sums_of(found_at(line, block), more_weights, more_slopes)
                    factors = (third[:, lanes], third[:, lanes], third_slope[:, lanes])
                    for dimension in range(3):
                        total = jnp.sum(sums[dimension] * factors[dimension], axis=0, keepdims=True)
                        out_ref[0, 0, dimension, pl.ds(first + block, 1), :] += (
                            -charge[:, lanes] * total
                        )


def sample(lay, starts, turns, atoms, waves, high, low):
    size = lay.lines_padded * lay.wave_rows
    field = pl.BlockSpec((1, size, LANES), lambda row, part, *refs: (row, 0, 0))
    shape = (lay.rows, lay.half_cols, 3, lay.blocks, LANES)
    return pl.pallas_call(
        functools.partial(sample_kernel, lay),
        grid_spec=pltpu.PrefetchScalarGridSpec(
            num_scalar_prefetch=2,
            grid=(lay.rows, lay.half_cols),
            in_specs=atom_specs(lay) + [field, field],
            out_specs=pl.BlockSpec((1, 1) + shape[2:], lambda row, part, *refs: (row, part, 0, 0, 0)),
        ),
        out_shape=jax.ShapeDtypeStruct(shape, jnp.float32),
        compiler_params=pltpu.CompilerParams(vmem_limit_bytes=40 * 1024 * 1024),
        cost_estimate=pl.CostEstimate(flops=10**10, bytes_accessed=10**7, transcendentals=0),
        name="sample",
    )(starts, turns, atoms, *waves, high, low)


def transform_kernel(
    lay,
    mesh_ref,
    *refs,
):
    message_refs = refs[: lay.rows]
    (
        first_high,
        first_low,
        second_high,
        second_low,
        back_high,
        back_low,
        last_high,
        last_low,
        out_high,
        out_low,
        field_ref,
        mine_ref,
        send_ref,
        recv_ref,
        home_ref,
        extra_ref,
        green_ref,
        send_sem,
        recv_sem,
        back_sem,
        home_sem,
        green_sem,
    ) = refs[lay.rows :]
    row = lax.axis_index("row")
    col = lax.axis_index("col")
    side = col % 2
    partner = (row, col + 1 - 2 * side)
    lines, length, own, padded = lay.lines, lay.length, lay.own, lay.slots_padded
    inner = lines - HALO

    number = message_number(lay, row, col)

    def green_copy(index):
        spot = lax.rem(index - number + lay.rows, lay.rows)
        return pltpu.make_async_copy(message_refs[index], green_ref.at[spot], green_sem.at[index])

    for index in range(lay.rows):
        green_copy(index).start()

    def three(high, low, table_high, table_low):
        return dot(high, table_high) + dot(low, table_high) + dot(high, table_low)

    def push(index):
        return pltpu.make_async_remote_copy(
            src_ref=send_ref.at[index],
            dst_ref=recv_ref.at[index],
            send_sem=send_sem.at[index],
            recv_sem=recv_sem.at[index],
            device_id=partner,
            device_id_type=MESH,
        )

    def push_back(index):
        return pltpu.make_async_remote_copy(
            src_ref=send_ref.at[index],
            dst_ref=home_ref.at[index],
            send_sem=back_sem.at[index],
            recv_sem=home_sem.at[index],
            device_id=partner,
            device_id_type=MESH,
        )

    def forward(slot):
        rows = [
            jnp.concatenate(
                [mesh_ref[r, pl.ds(start, lines, stride=lay.stride), :] for r in range(lay.rows)],
                axis=1,
            )
            for start in (slot, padded + slot)
        ]
        high, low = halves_of(jnp.concatenate(rows, axis=0))
        found = three(high, low, first_high[...], first_low[...])
        upper, lower = found[:lines], found[lines:]
        return upper[:, :length], upper[:, length:], lower[:, :length], lower[:, length:]

    for base, target in ((0, send_ref), (own, mine_ref)):
        away = base == 0

        @pl.loop(0, own)
        def first_pass(i):
            real_cos, real_sin, imag_cos, imag_sin = forward(base + i)

            @pl.when(i == 0)
            def mirrored():
                target[own, 0] = real_cos - imag_sin
                target[own, 1] = -imag_cos - real_sin

            target[i, 0] = real_cos + imag_sin
            target[i, 1] = imag_cos - real_sin
            if away:

                @pl.when(i == 0)
                def start_mirrored():
                    push(own).start()

                push(i).start()

    @pl.loop(0, own + 1)
    def sent(i):
        push(i).wait_send()

    for index in range(lay.rows):
        green_copy(index).wait()

    def spectrum(index):
        mine, other = mine_ref[index], recv_ref[index]
        parts = []
        for part in range(2):
            a, b = mine[part], other[part]
            parts.append(
                jnp.concatenate(
                    [
                        a[HALO:inner],
                        a[inner:] + b[:HALO],
                        b[HALO:inner],
                        b[inner:] + a[:HALO],
                    ],
                    axis=0,
                )
            )
        high, low = halves_of(jnp.concatenate(parts, axis=1))
        found = (
            dot(second_high[...], high) + dot(second_high[...], low) + dot(second_low[...], high)
        )
        cos_part, sin_part = found[:length], found[length:]
        real = cos_part[:, :length] + sin_part[:, length:]
        imag = cos_part[:, length:] - sin_part[:, :length]
        blocks = [green_ref[r, index] for r in range(lay.rows)]
        green = jnp.concatenate(blocks, axis=0)
        return real * green, imag * green

    push(own).wait_recv()
    extra_ref[0], extra_ref[1] = spectrum(own)

    @pl.loop(0, own)
    def second_pass(i):
        push(i).wait_recv()
        real, imag = spectrum(i)
        first = jnp.where(i == 0, 1.0, 0.0)
        real += first * extra_ref[0]
        imag += first * extra_ref[1]
        high, low = halves_of(jnp.concatenate([real, imag], axis=1))
        found = dot(back_high[...], high) + dot(back_high[...], low) + dot(back_low[...], high)
        cos_part, sin_part = found[: 2 * lines], found[2 * lines :]
        real = cos_part[:, :length] - sin_part[:, length:]
        imag = cos_part[:, length:] + sin_part[:, :length]
        mine_ref[i, 0] = real[:lines]
        mine_ref[i, 1] = imag[:lines]
        send_ref[i, 0] = real[lines:]
        send_ref[i, 1] = imag[lines:]
        push_back(i).start()

    cleared = 0 if lay.slots < padded else lines * lay.stride // 8 * 8
    total_rows = mesh_ref.shape[1]
    for r in range(lay.rows):
        field_ref[r, pl.ds(cleared, total_rows - cleared), :] = jnp.zeros(
            (total_rows - cleared, LANES), jnp.float32
        )

    def last(local, planes_ref, i):
        high, low = halves_of(jnp.concatenate([planes_ref[i, 0], planes_ref[i, 1]], axis=0))
        found = three(high, low, last_high[...], last_low[...])
        width = lay.rows * LANES
        real = found[:lines, :width] - found[lines:, width:]
        imag = found[:lines, width:] + found[lines:, :width]
        for part, value in enumerate((real, imag)):
            where = pl.ds(part * padded + local, lines, stride=lay.stride)
            for r in range(lay.rows):
                field_ref[r, where, :] = value[:, r * LANES : (r + 1) * LANES]

    @pl.loop(0, own)
    def last_mine(i):
        last(own + i, mine_ref, i)

    @pl.loop(0, own)
    def last_home(i):
        push_back(i).wait_recv()
        last(i, home_ref, i)

    @pl.loop(0, lay.lines_padded)
    def split(line):
        where = pl.ds(pl.multiple_of(line * lay.wave_rows, lay.wave_rows), lay.wave_rows)
        for r in range(lay.rows):
            value = field_ref[r, pl.ds(line * lay.stride, lay.wave_rows), :]
            out_high[r, where, :], out_low[r, where, :] = halves_of(value)

    @pl.loop(0, own)
    def returned(i):
        push_back(i).wait_send()


def message_number(lay, row, col):
    member = lax.rem(row, lay.group)
    frame = row // lay.group
    return (lax.rem(col, 2) * lay.frames + frame) * lay.splits + lax.rem(member, lay.splits)


def transform(lay, mesh, messages, tables):
    dma = pltpu.SemaphoreType.DMA
    plane = (2, lay.lines, lay.length)
    vmem = pl.BlockSpec(memory_space=pltpu.VMEM)
    out = jax.ShapeDtypeStruct(
        (lay.rows, lay.lines_padded * lay.wave_rows, LANES), jnp.bfloat16
    )
    return pl.pallas_call(
        functools.partial(transform_kernel, lay),
        in_specs=[vmem] + [pl.BlockSpec(memory_space=pl.ANY)] * lay.rows + [vmem] * len(tables),
        out_specs=[vmem, vmem],
        out_shape=[out, out],
        scratch_shapes=[
            pltpu.VMEM(mesh.shape, jnp.float32),
            pltpu.VMEM((lay.own + 1,) + plane, jnp.float32),
            pltpu.VMEM((lay.own + 1,) + plane, jnp.float32),
            pltpu.VMEM((lay.own + 1,) + plane, jnp.float32),
            pltpu.VMEM((lay.own,) + plane, jnp.float32),
            pltpu.VMEM((2, lay.length, lay.length), jnp.float32),
            pltpu.VMEM((lay.rows,) + messages[0].shape, jnp.float32),
            dma((lay.own + 1,)),
            dma((lay.own + 1,)),
            dma((lay.own,)),
            dma((lay.own,)),
            dma((lay.rows,)),
        ],
        compiler_params=pltpu.CompilerParams(
            has_side_effects=True, vmem_limit_bytes=62 * 1024 * 1024
        ),
        cost_estimate=pl.CostEstimate(flops=10**10, bytes_accessed=10**7, transcendentals=0),
        name="transform",
    )(mesh, *messages, *tables)


def table_halves(value):
    leading = lax.reduce_precision(value, exponent_bits=8, mantissa_bits=7)
    return leading.astype(jnp.bfloat16), (value - leading).astype(jnp.bfloat16)


def constant_halves(value):
    high = value.astype(jnp.bfloat16)
    return high, (value - high.astype(np.float64)).astype(jnp.bfloat16)


def make_tables(lay):
    length, half = lay.length, lay.half_cols * lay.block_cols
    waves = np.arange(length)
    spots = np.arange(LANES)
    across = (np.arange(lay.rows)[:, None] * lay.block_rows + spots[None, :] - HALO).reshape(-1)
    valid = np.tile(spots < lay.span, lay.rows)
    angle = across[:, None] * waves[None, :] % length * (2.0 * np.pi / length)
    cosine = np.where(valid[:, None], np.cos(angle), 0.0)
    sine = np.where(valid[:, None], np.sin(angle), 0.0)
    first = constant_halves(np.concatenate([cosine, sine], axis=1))
    last = constant_halves(np.concatenate([cosine.T, sine.T], axis=1))
    zero = lax.optimization_barrier(jnp.int32(0))
    waves = jnp.arange(length, dtype=jnp.int32)
    second = jnp.concatenate(phases(waves[:, None] * (waves[None, :] + zero), length), axis=0)
    near = jnp.arange(lay.lines, dtype=jnp.int32) - HALO + length + zero
    both = jnp.concatenate([near, near + half])
    back = jnp.concatenate(phases(both[:, None] * waves[None, :], length), axis=0)
    tables = []
    for pair in (first, table_halves(second), table_halves(back), last):
        tables.extend(pair)
    return tables


def make_waves(lay, row, col, side):
    length = lay.length
    member = row % lay.group
    source = 2 * (col // 2) + member // lay.splits
    split = member % lay.splits
    start = lay.block_cols * source + jnp.where(source >= lay.half_cols, 1, 0) + split * lay.slots
    index = jnp.arange(lay.slots_padded, dtype=jnp.int32)
    slot = jnp.where(index < lay.own, (1 - side) * lay.own, side * lay.own) + index % lay.own
    waves = start + slot
    packed = (source == 0) & (split == 0) & (slot == 0) & (index < lay.slots)
    live = (index < lay.slots)[None, :, None]
    offsets = jnp.arange(6, dtype=jnp.int32)
    cosine, sine = phases(offsets[:, None] * waves[None, :], length)
    shape = (lay.slots_padded, LANES)
    cosines = jnp.broadcast_to(jnp.where(live, cosine[:, :, None], 0.0), (6,) + shape)
    sines = jnp.broadcast_to(jnp.where(live, sine[:, :, None], 0.0), (6,) + shape)
    return (
        jnp.broadcast_to(waves[:, None], shape),
        jnp.broadcast_to(packed[:, None].astype(jnp.float32), shape),
        cosines,
        sines,
    )


def share_green(lay, influence, row, col):
    length = lay.length
    rows, cols = lay.rows, lay.cols
    scale = 1.0 / float(length) ** 3
    used = lay.block_cols // 2
    offset = jnp.where(col >= lay.half_cols, 1, 0)
    middle = lax.ppermute(influence[:, 0, :], "col", [(lay.half_cols, 0)])
    block = lax.dynamic_slice_in_dim(influence, offset, used, axis=1).transpose(1, 0, 2)
    block = block.reshape(lay.splits, 2, lay.own, lay.block_rows, length)
    special = col == 0
    zeroth = block[0, 0, 0]
    extra = jnp.where(special, (0.5 * scale) * (zeroth - middle), 0.0)
    zeroth = jnp.where(special, (0.5 * scale) * (zeroth + middle), (2.0 * scale) * zeroth)
    block = jnp.concatenate([(2.0 * scale) * block, jnp.zeros_like(block[:, :, :1])], axis=2)
    block = block.at[0, 0, 0].set(zeroth).at[0, 0, lay.own].set(extra)
    block = block.reshape((2 * lay.splits,) + block.shape[2:])
    messages = []
    for number in range(rows):
        message = (number - row) % rows
        split = message % lay.splits
        side = message // (lay.frames * lay.splits)
        sent = lax.dynamic_index_in_dim(block, split * 2 + side, keepdims=False)
        pairs = []
        for r in range(rows):
            at = (number - r) % rows
            to_split, rest = at % lay.splits, at // lay.splits
            to_frame, to_side = rest % lay.frames, rest // lay.frames
            for c in range(cols):
                to_row = to_frame * lay.group + (c % 2) * lay.splits + to_split
                pairs.append((r * cols + c, to_row * cols + 2 * (c // 2) + to_side))
        messages.append(lax.ppermute(sent, ("row", "col"), pairs))
    return messages


def forces_of(cell_index, fraction, charge, atom_count, influence):
    frames, _, atoms = fraction.shape
    lay = Layout(frames, influence.shape[2], atoms)
    row = lax.axis_index("row")
    col = lax.axis_index("col")
    side = col % 2
    messages = share_green(lay, influence, row, col)
    tables = make_tables(lay)
    waves = make_waves(lay, row, col, side)

    slot_ids = jnp.arange(atoms, dtype=jnp.int32)
    alive = slot_ids[None, :] < atom_count
    charges = jnp.where(alive, charge, 0.0)
    origin = jnp.stack([row * lay.block_rows, (col // lay.half_cols) * lay.half_cols * lay.block_cols, 0])
    cells = cell_index - origin[None, :, None]
    payload = jnp.concatenate(
        [
            cells.astype(jnp.float32),
            fraction,
            charges[:, None, :],
            alive[:, None, :].astype(jnp.float32),
        ],
        axis=1,
    )
    sorted_atoms, rank = sort_atoms(lay, payload)
    shared = gather_atoms(lay, sorted_atoms)

    lines = shared[:, :, 1, :].reshape(lay.rows * lay.half_cols * lay.blocks, LANES)
    lives = shared[:, :, 7, :].reshape(lines.shape) > 0.5
    lowest = jnp.min(jnp.where(lives, lines, 1024.0), axis=1).astype(jnp.int32)
    highest = jnp.max(jnp.where(lives, lines, -1024.0), axis=1).astype(jnp.int32)
    live = highest >= lowest
    starts = jnp.where(live, lowest + HALO - 5, 0)
    turns = jnp.where(live, (highest - lowest + 6 + CHUNK - 1) // CHUNK, 0)

    mesh = spread(lay, starts, turns, shared, waves)
    high, low = transform(lay, mesh, messages, tables)
    partial = sample(lay, starts, turns, shared, waves, high, low)
    returned = return_forces(lay, partial)
    forces = jnp.sum(returned, axis=1).reshape(frames, 3, atoms)
    forces = jnp.pad(forces, ((0, 0), (0, 5), (0, 0)))
    return unsort_forces(rank, forces)[:, :3]


def solution(mesh):
    placed = (
        P(None, None, ("row", "col")),
        P(None, None, ("row", "col")),
        P(None, ("row", "col")),
        P(None, ("row", "col")),
        P("row", "col", None),
    )
    return jax.shard_map(
        forces_of, mesh=mesh, in_specs=placed, out_specs=P(None, None, ("row", "col")), check_vma=False
    )
```

```python
import functools
import math

import jax
import jax.numpy as jnp
import numpy as np
from jax import lax
from jax.experimental import pallas as pl
from jax.experimental.pallas import tpu as pltpu
from jax.sharding import PartitionSpec as P


MESH = pl.DeviceIdType.MESH
LANES = 128
CHUNK = 10
PACK = 4
HALO = 8
NT = (((1,), (1,)), ((), ()))
NN = (((1,), (0,)), ((), ()))


def dot(left, right, form=NN):
    return lax.dot_general(left, right, form, preferred_element_type=jnp.float32)


def halves_of(value):
    high = value.astype(jnp.bfloat16)
    return high, (value - high.astype(jnp.float32)).astype(jnp.bfloat16)


def spline_rows(fraction):
    nothing = jnp.zeros_like(fraction)
    levels = [fraction, 1.0 - fraction]
    slopes = levels
    for degree in range(3, 7):
        padded = levels + [nothing]
        following = []
        for offset in range(degree):
            beneath = padded[offset - 1] if offset > 0 else nothing
            following.append(
                ((fraction + offset) * padded[offset] + (degree - fraction - offset) * beneath)
                * (1.0 / (degree - 1))
            )
        if degree == 6:
            slopes = [
                padded[offset] - (padded[offset - 1] if offset > 0 else nothing)
                for offset in range(6)
            ]
        levels = following
    return levels, slopes


def dense(distance, lists):
    results = [jnp.zeros(distance.shape, jnp.float32) for _ in lists]
    for offset in range(6):
        hit = distance == offset
        results = [jnp.where(hit, rows[offset], result) for rows, result in zip(lists, results)]
    return results


def row_of(lists, dimension):
    starts = range(dimension, lists[0].shape[0], 3)
    return [
        jnp.concatenate([entry[start : start + 1, :] for start in starts], axis=1)
        for entry in lists
    ]


def phases(product, length):
    half = length // 2
    moved = product + half
    if length & (length - 1):
        turned = lax.rem(moved, length) - half
    else:
        turned = (moved & (length - 1)) - half
    angle = turned.astype(jnp.float32) * (2.0 * math.pi / length / 4.0)
    square = angle * angle
    sine = angle * (
        1.0
        + square
        * (-1.0 / 6 + square * (1.0 / 120 + square * (-1.0 / 5040 + square * (1.0 / 362880))))
    )
    cosine = 1.0 + square * (
        -0.5
        + square
        * (1.0 / 24 + square * (-1.0 / 720 + square * (1.0 / 40320 - square * (1.0 / 3628800))))
    )
    for _ in range(2):
        sine, cosine = 2.0 * sine * cosine, 1.0 - 2.0 * sine * sine
    return cosine, sine


def wave_rows(cosine, sine, cos_ref, sin_ref, packed_ref, cells, rows):
    copies = cosine.shape[1] // LANES

    def wide(ref, offset):
        return jnp.concatenate([ref[offset]] * copies, axis=1) * rows[offset]

    even, odd = wide(cos_ref, 0), wide(sin_ref, 0)
    for offset in range(1, 6):
        even += wide(cos_ref, offset)
        odd += wide(sin_ref, offset)
    real = cosine * even + sine * odd
    imag = cosine * odd - sine * even
    middle = rows[0] - rows[1] + rows[2] - rows[3] + rows[4] - rows[5]
    middle = jnp.where((cells & 1) == 0, middle, -middle)
    packed = jnp.concatenate([packed_ref[...]] * copies, axis=1)
    return jnp.concatenate([real, jnp.where(packed > 0.5, middle, imag)], axis=0)


def sort_kernel(bins, width, payload_ref, sorted_ref, rank_ref):
    atoms = payload_ref.shape[2]
    blocks = atoms // LANES
    line = payload_ref[0, 1:2, :]
    line = line - width * jnp.floor((line + 0.5) * (1.0 / width))
    line = jnp.where(payload_ref[0, 7:8, :] > 0.5, line.astype(jnp.int32), bins - 1)
    kinds = lax.broadcasted_iota(jnp.int32, (bins, LANES), 0)
    marks = [jnp.where(line[:, lanes_of(block)] == kinds, 1.0, 0.0) for block in range(blocks)]
    across = lax.broadcasted_iota(jnp.int32, (LANES, LANES), 0)
    down = lax.broadcasted_iota(jnp.int32, (LANES, LANES), 1)
    before = jnp.where(across < down, 1.0, 0.0).astype(jnp.bfloat16)
    every = jnp.ones((LANES, LANES), jnp.bfloat16)
    packed = jnp.concatenate(marks, axis=0).astype(jnp.bfloat16)
    earlier = dot(packed, before)
    counts = dot(packed, every)
    running = jnp.zeros((bins, LANES), jnp.float32)
    partial = []
    for block in range(blocks):
        partial.append(running + earlier[block * bins : (block + 1) * bins])
        running += counts[block * bins : (block + 1) * bins]
    lower = lax.broadcasted_iota(jnp.int32, (bins, bins), 1) < lax.broadcasted_iota(
        jnp.int32, (bins, bins), 0
    )
    lower = jnp.where(lower, 1.0, 0.0).astype(jnp.bfloat16)
    high, low = halves_of(running)
    base = dot(lower, high) + dot(lower, low)
    for block in range(blocks):
        places = marks[block] * (partial[block] + base)
        rank_ref[0, :, block * LANES : (block + 1) * LANES] = jnp.sum(places, axis=0, keepdims=True)

    value = payload_ref[0]
    first, rest = halves_of(value)
    left = value - first.astype(jnp.float32)
    third = (left - rest.astype(jnp.float32)).astype(jnp.bfloat16)
    pieces = jnp.concatenate([first, rest, third, jnp.zeros_like(first)], axis=0)
    rank = rank_ref[0].astype(jnp.int32)
    size = math.gcd(256, atoms)

    @pl.loop(0, atoms // size)
    def place(part):
        start = pl.multiple_of(part * size, size)
        spots = lax.broadcasted_iota(jnp.int32, (size, atoms), 0) + start
        chosen = jnp.where(rank == spots, 1.0, 0.0).astype(jnp.bfloat16)
        moved = dot(pieces, chosen, NT)
        sorted_ref[0, :, pl.ds(start, size)] = moved[0:8] + moved[8:16] + moved[16:24]


def sort_atoms(lay, payload):
    frames, rows, atoms = payload.shape
    whole = lambda frame: (frame, 0, 0)
    bins = -(-(lay.block_cols + 1) // 16) * 16
    return pl.pallas_call(
        functools.partial(sort_kernel, bins, lay.block_cols),
        grid=(frames,),
        in_specs=[pl.BlockSpec((1, rows, atoms), whole)],
        out_specs=[pl.BlockSpec((1, rows, atoms), whole), pl.BlockSpec((1, 1, atoms), whole)],
        out_shape=[
            jax.ShapeDtypeStruct((frames, rows, atoms), jnp.float32),
            jax.ShapeDtypeStruct((frames, 1, atoms), jnp.float32),
        ],
        compiler_params=pltpu.CompilerParams(vmem_limit_bytes=32 * 1024 * 1024),
        name="sort_atoms",
    )(payload)


def unsort_kernel(rank_ref, force_ref, out_ref):
    atoms = rank_ref.shape[2]
    value = force_ref[0]
    high, low = halves_of(value)
    left = value - high.astype(jnp.float32)
    third = (left - low.astype(jnp.float32)).astype(jnp.bfloat16)
    pieces = jnp.concatenate([high, low, third, jnp.zeros_like(high)], axis=0)
    rank = rank_ref[0].astype(jnp.int32)
    width = math.gcd(256, atoms)

    @pl.loop(0, atoms // width)
    def place(part):
        start = pl.multiple_of(part * width, width)
        spots = lax.broadcasted_iota(jnp.int32, (atoms, width), 0)
        lanes = pl.ds(start, width)
        here = rank_ref[0, :, lanes].astype(jnp.int32)
        chosen = jnp.where(here == spots, 1.0, 0.0).astype(jnp.bfloat16)
        moved = dot(pieces, chosen, NN)
        out_ref[0, :, lanes] = moved[0:8] + moved[8:16] + moved[16:24]


def unsort_forces(rank, forces):
    frames, rows, atoms = forces.shape
    whole = lambda frame: (frame, 0, 0)
    return pl.pallas_call(
        unsort_kernel,
        grid=(frames,),
        in_specs=[pl.BlockSpec((1, 1, atoms), whole), pl.BlockSpec((1, rows, atoms), whole)],
        out_specs=pl.BlockSpec((1, rows, atoms), whole),
        out_shape=jax.ShapeDtypeStruct((frames, rows, atoms), jnp.float32),
        compiler_params=pltpu.CompilerParams(vmem_limit_bytes=32 * 1024 * 1024),
        name="unsort_forces",
    )(rank, forces)


class Layout:
    def __init__(self, frames, length, atoms):
        self.rows = lax.axis_size("row")
        self.cols = lax.axis_size("col")
        self.frames = frames
        self.length = length
        self.atoms = atoms
        self.group = self.rows // frames
        self.half_cols = self.cols // 2
        self.block_rows = length // self.rows
        self.block_cols = length // self.cols
        self.slots = length // 2 // (self.group * self.half_cols)
        self.own = self.slots // 2
        self.slots_padded = max(8, self.slots)
        self.wave_rows = 2 * self.slots_padded
        self.stride = self.wave_rows + 1
        self.lines = self.half_cols * self.block_cols + HALO
        self.lines_padded = -(-(self.lines + CHUNK - 1) // 8) * 8
        self.splits = self.group // 2
        self.blocks = atoms // LANES
        self.span = self.block_rows + HALO
        self.pack = math.gcd(PACK, self.blocks)


def gather_kernel(lay, mine_ref, all_ref, local_sem, send_sem, recv_sem, pass_sem, took_sem):
    row = lax.axis_index("row")
    col = lax.axis_index("col")
    pair = col // 2
    side = col % 2
    half = col // lay.half_cols
    place = col % lay.half_cols
    hub = half == side
    pair_start = (2 * pair) % lay.half_cols

    def nearest(step):
        other = lax.rem(row // lay.group + step // lay.group, lay.frames)
        return other * lay.group + lax.rem(row + step, lay.group)

    def first_send(frame, member):
        target = frame * lay.group + member
        index = frame * lay.group + member
        return target, pltpu.make_async_remote_copy(
            src_ref=mine_ref.at[frame],
            dst_ref=all_ref.at[row, place],
            send_sem=send_sem.at[index],
            recv_sem=recv_sem.at[row, side],
            device_id=(target, 2 * pair + half),
            device_id_type=MESH,
        )

    def self_copy(frame):
        return pltpu.make_async_copy(mine_ref.at[frame], all_ref.at[row, place], local_sem)

    for frame in range(lay.frames):
        for member in range(lay.group):
            target, copy = first_send(frame, member)
            alone = (target == row) & hub

            @pl.when(jnp.logical_not(alone))
            def send():
                copy.start()

            @pl.when(alone)
            def keep():
                self_copy(frame).start()

    def second_send(source, part, other):
        spot = pair_start + part
        return pltpu.make_async_remote_copy(
            src_ref=all_ref.at[source, spot],
            dst_ref=all_ref.at[source, spot],
            send_sem=pass_sem.at[source, part, other - 1],
            recv_sem=took_sem.at[source, spot],
            device_id=(row, 2 * ((pair + other) % lay.half_cols) + side),
            device_id_type=MESH,
        )

    def arrival(source, spot, sem):
        return pltpu.make_async_remote_copy(
            src_ref=all_ref.at[source, spot],
            dst_ref=all_ref.at[source, spot],
            send_sem=send_sem.at[0],
            recv_sem=sem,
            device_id=(row, col),
            device_id_type=MESH,
        )

    @pl.when(hub)
    def forward():
        for step in range(lay.rows):
            source = nearest(step)
            for part in range(2):
                spot = pair_start + part
                alone = (source == row) & (part == side)

                @pl.when(jnp.logical_not(alone))
                def landed():
                    arrival(source, spot, recv_sem.at[source, part]).wait_recv()

                @pl.when(alone)
                def kept():
                    self_copy(row // lay.group).wait()

                for other in range(1, lay.half_cols):
                    second_send(source, part, other).start()

    for frame in range(lay.frames):
        for member in range(lay.group):
            target, copy = first_send(frame, member)

            @pl.when(jnp.logical_not((target == row) & hub))
            def sent():
                copy.wait_send()

    for spot in range(lay.half_cols):
        local = hub & (pair == side * (lay.half_cols // 2) + spot // 2)

        @pl.when(jnp.logical_not(local))
        def took():
            for source in range(lay.rows):
                arrival(source, spot, took_sem.at[source, spot]).wait_recv()

    @pl.when(hub)
    def passed():
        for source in range(lay.rows):
            for part in range(2):
                for other in range(1, lay.half_cols):
                    second_send(source, part, other).wait_send()


def gather_atoms(lay, mine):
    _, rows, atoms = mine.shape
    dma = pltpu.SemaphoreType.DMA
    return pl.pallas_call(
        functools.partial(gather_kernel, lay),
        in_specs=[pl.BlockSpec(memory_space=pltpu.VMEM)],
        out_specs=pl.BlockSpec(memory_space=pltpu.VMEM),
        out_shape=jax.ShapeDtypeStruct((lay.rows, lay.half_cols, rows, atoms), jnp.float32),
        scratch_shapes=[
            dma,
            dma((lay.rows,)),
            dma((lay.rows, 2)),
            dma((lay.rows, 2, lay.half_cols - 1)),
            dma((lay.rows, lay.half_cols)),
        ],
        compiler_params=pltpu.CompilerParams(has_side_effects=True),
        name="gather_atoms",
    )(mine)


def return_kernel(lay, force_ref, out_ref, local_sem, send_sem, recv_sem):
    row = lax.axis_index("row")
    col = lax.axis_index("col")
    side = col % 2
    frame = row // lay.group
    index = (row % lay.group) * lay.half_cols + col // 2
    copies = []
    for source in range(lay.rows):
        for spot in range(lay.half_cols):
            owner = side * lay.half_cols + spot
            copies.append(
                (
                    (source == row) & (owner == col),
                    pltpu.make_async_remote_copy(
                        src_ref=force_ref.at[source, spot],
                        dst_ref=out_ref.at[frame, index],
                        send_sem=send_sem.at[source, spot],
                        recv_sem=recv_sem.at[frame, index],
                        device_id=(source, owner),
                        device_id_type=MESH,
                    ),
                    pltpu.make_async_copy(
                        force_ref.at[source, spot], out_ref.at[frame, index], local_sem
                    ),
                )
            )
    for alone, copy, local in copies:

        @pl.when(jnp.logical_not(alone))
        def send():
            copy.start()

        @pl.when(alone)
        def keep():
            local.start()

    for alone, copy, local in copies:

        @pl.when(jnp.logical_not(alone))
        def sent():
            copy.wait_send()

        @pl.when(alone)
        def kept():
            local.wait()

    half = col // lay.half_cols
    for from_frame in range(lay.frames):
        for member in range(lay.group):
            for pair in range(lay.half_cols):
                slot = member * lay.half_cols + pair
                alone = (from_frame * lay.group + member == row) & (2 * pair + half == col)

                @pl.when(jnp.logical_not(alone))
                def landed():
                    pltpu.make_async_remote_copy(
                        src_ref=out_ref.at[from_frame, slot],
                        dst_ref=out_ref.at[from_frame, slot],
                        send_sem=send_sem.at[0, 0],
                        recv_sem=recv_sem.at[from_frame, slot],
                        device_id=(row, col),
                        device_id_type=MESH,
                    ).wait_recv()


def return_forces(lay, forces):
    rows, half_cols = forces.shape[:2]
    members = lay.group * half_cols
    dma = pltpu.SemaphoreType.DMA
    return pl.pallas_call(
        functools.partial(return_kernel, lay),
        in_specs=[pl.BlockSpec(memory_space=pltpu.VMEM)],
        out_specs=pl.BlockSpec(memory_space=pltpu.VMEM),
        out_shape=jax.ShapeDtypeStruct((lay.frames, members) + forces.shape[2:], jnp.float32),
        scratch_shapes=[dma, dma((rows, half_cols)), dma((lay.frames, members))],
        compiler_params=pltpu.CompilerParams(has_side_effects=True),
        name="return_forces",
    )(forces)


def atom_group(lay, atoms_ref, waves_ref, group, with_slopes):
    width = lay.pack * LANES
    lanes = pl.ds(pl.multiple_of(group * width, width), width)
    piece = atoms_ref[0, 0, :, lanes]
    cells = piece[0:3].astype(jnp.int32)
    packed = [piece[3:6, lanes_of(block)] for block in range(lay.pack)]
    values, slopes = spline_rows(jnp.concatenate(packed, axis=0))
    charge = piece[6:7]
    spots = lax.broadcasted_iota(jnp.int32, (lay.span, width), 0)
    kinds = [values, slopes] if with_slopes else [values]
    wide = dense(cells[0:1] + HALO - spots, [row_of(kind, 0) for kind in kinds])
    pad = jnp.zeros((LANES - lay.span, width), jnp.float32)
    wide = [jnp.concatenate([entry, pad], axis=0) for entry in wide]
    turned = jnp.concatenate([waves_ref[...]] * lay.pack, axis=1) * cells[2:3]
    cosine, sine = phases(turned, lay.length)
    return cells, kinds, charge, wide, cosine, sine


def line_weights(cells, kinds, starts):
    lines = lax.broadcasted_iota(jnp.int32, (-(-CHUNK // 8) * 8, LANES), 0)
    lines = jnp.concatenate([lines + start for start in starts], axis=1)
    return dense(cells[1:2] + HALO - lines, [row_of(kind, 1) for kind in kinds])


def lanes_of(block):
    return slice(block * LANES, (block + 1) * LANES)


def pick(kinds, block):
    return [[row[3 * block : 3 * block + 3] for row in kind] for kind in kinds]


def rows_at(lay, line):
    return pl.ds(pl.multiple_of(line * lay.wave_rows, lay.wave_rows), CHUNK * lay.wave_rows)


def spread_kernel(
    lay, starts_ref, turns_ref, atoms_ref, waves_ref, packed_ref, cos_ref, sin_ref, mesh_ref
):
    part = pl.program_id(1)
    pencil = pl.program_id(0) * lay.half_cols + part

    @pl.when(part == 0)
    def clear():
        mesh_ref[...] = jnp.zeros_like(mesh_ref)

    @pl.loop(0, lay.blocks // lay.pack)
    def add_group(group):
        base = pencil * lay.blocks + group * lay.pack

        @pl.when(turns_ref[base] > 0)
        def live():
            cells, kinds, charge, wide, cosine, sine = atom_group(
                lay, atoms_ref, waves_ref, group, False
            )
            tables = cosine, sine, cos_ref, sin_ref, packed_ref
            waves = wave_rows(*tables, cells[2:3], row_of(kinds[0], 2)) * charge
            starts = [starts_ref[base + block] for block in range(lay.pack)]
            (weights,) = line_weights(cells, kinds, starts)
            rights = []
            for block in range(lay.pack):
                high, low = halves_of(wide[0][:, lanes_of(block)])
                rights.append(
                    jnp.concatenate(
                        [
                            jnp.concatenate([high, high], axis=1),
                            jnp.concatenate([low, low], axis=1),
                        ],
                        axis=0,
                    )
                )

            def total_of(weights, block):
                wave = waves[:, lanes_of(block)]
                product = jnp.concatenate([weights[i : i + 1] * wave for i in range(CHUNK)], axis=0)
                high, low = halves_of(product)
                total = dot(jnp.concatenate([high, low], axis=1), rights[block], NT)
                return total[:, :LANES] + total[:, LANES:]

            totals = [total_of(weights[:, lanes_of(block)], block) for block in range(lay.pack)]

            def add(line, total):
                for i in range(CHUNK):
                    part = total[i * lay.wave_rows : (i + 1) * lay.wave_rows]
                    mesh_ref[0, pl.ds((line + i) * lay.stride, lay.wave_rows), :] += part

            for block in range(lay.pack):
                add(starts[block], totals[block])
            for block in range(lay.pack):

                @pl.loop(1, turns_ref[base + block])
                def more(turn):
                    line = starts[block] + turn * CHUNK
                    lanes = lanes_of(block)
                    (weights,) = line_weights(cells[:, lanes], pick(kinds, block), [line])
                    add(line, total_of(weights, block))


def atom_specs(lay):
    fixed = lambda row, part, *refs: (0, 0, 0)
    return [
        pl.BlockSpec((1, 1, 8, lay.atoms), lambda row, part, *refs: (row, part, 0, 0)),
        pl.BlockSpec((lay.slots_padded, LANES), lambda row, part, *refs: (0, 0)),
        pl.BlockSpec((lay.slots_padded, LANES), lambda row, part, *refs: (0, 0)),
        pl.BlockSpec((6, lay.slots_padded, LANES), fixed),
        pl.BlockSpec((6, lay.slots_padded, LANES), fixed),
    ]


def spread(lay, starts, turns, atoms, waves):
    size = -(-lay.lines_padded * lay.stride // 8) * 8
    return pl.pallas_call(
        functools.partial(spread_kernel, lay),
        grid_spec=pltpu.PrefetchScalarGridSpec(
            num_scalar_prefetch=2,
            grid=(lay.rows, lay.half_cols),
            in_specs=atom_specs(lay),
            out_specs=pl.BlockSpec((1, size, LANES), lambda row, part, *refs: (row, 0, 0)),
        ),
        out_shape=jax.ShapeDtypeStruct((lay.rows, size, LANES), jnp.float32),
        compiler_params=pltpu.CompilerParams(vmem_limit_bytes=40 * 1024 * 1024),
        cost_estimate=pl.CostEstimate(flops=10**10, bytes_accessed=10**7, transcendentals=0),
        name="spread",
    )(starts, turns, atoms, *waves)


def sample_kernel(
    lay,
    starts_ref,
    turns_ref,
    atoms_ref,
    waves_ref,
    packed_ref,
    cos_ref,
    sin_ref,
    high_ref,
    low_ref,
    out_ref,
):
    pencil = pl.program_id(0) * lay.half_cols + pl.program_id(1)

    @pl.loop(0, lay.blocks // lay.pack)
    def sample_group(group):
        base = pencil * lay.blocks + group * lay.pack
        first = group * lay.pack

        @pl.when(turns_ref[base] == 0)
        def idle():
            for block in range(lay.pack):
                out_ref[0, 0, :, pl.ds(first + block, 1), :] = jnp.zeros((3, 1, LANES), jnp.float32)

        @pl.when(turns_ref[base] > 0)
        def live():
            cells, kinds, charge, wide, cosine, sine = atom_group(
                lay, atoms_ref, waves_ref, group, True
            )
            tables = cosine, sine, cos_ref, sin_ref, packed_ref
            third = wave_rows(*tables, cells[2:3], row_of(kinds[0], 2))
            third_slope = wave_rows(*tables, cells[2:3], row_of(kinds[1], 2))
            starts = [starts_ref[base + block] for block in range(lay.pack)]
            weights, weight_slopes = line_weights(cells, kinds, starts)
            rights = []
            for block in range(lay.pack):
                both = jnp.concatenate([entry[:, lanes_of(block)] for entry in wide], axis=1)
                high, low = halves_of(both)
                rights.append((jnp.concatenate([high, high], axis=0), low))

            def found_at(line, block):
                where = rows_at(lay, line)
                field_high = high_ref[0, where, :]
                field = jnp.concatenate([field_high, low_ref[0, where, :]], axis=1)
                right, low = rights[block]
                return dot(field, right) + dot(field_high, low)

            def sums_of(found, weights, weight_slopes):
                plain = sloped = across = jnp.zeros((lay.wave_rows, LANES), jnp.float32)
                for i in range(CHUNK):
                    lines = slice(i * lay.wave_rows, (i + 1) * lay.wave_rows)
                    value = found[lines, :LANES]
                    plain += value * weights[i : i + 1]
                    across += value * weight_slopes[i : i + 1]
                    sloped += found[lines, LANES:] * weights[i : i + 1]
                return sloped, across, plain

            founds = [found_at(starts[block], block) for block in range(lay.pack)]
            for block in range(lay.pack):
                lanes = lanes_of(block)
                sums = sums_of(founds[block], weights[:, lanes], weight_slopes[:, lanes])
                factors = (third[:, lanes], third[:, lanes], third_slope[:, lanes])
                for dimension in range(3):
                    total = jnp.sum(sums[dimension] * factors[dimension], axis=0, keepdims=True)
                    out_ref[0, 0, dimension, pl.ds(first + block, 1), :] = -charge[:, lanes] * total
            for block in range(lay.pack):

                @pl.loop(1, turns_ref[base + block])
                def more(turn):
                    line = starts[block] + turn * CHUNK
                    lanes = lanes_of(block)
                    more_weights, more_slopes = line_weights(
                        cells[:, lanes], pick(kinds, block), [line]
                    )
                    sums = sums_of(found_at(line, block), more_weights, more_slopes)
                    factors = (third[:, lanes], third[:, lanes], third_slope[:, lanes])
                    for dimension in range(3):
                        total = jnp.sum(sums[dimension] * factors[dimension], axis=0, keepdims=True)
                        out_ref[0, 0, dimension, pl.ds(first + block, 1), :] += (
                            -charge[:, lanes] * total
                        )


def sample(lay, starts, turns, atoms, waves, high, low):
    size = lay.lines_padded * lay.wave_rows
    field = pl.BlockSpec((1, size, LANES), lambda row, part, *refs: (row, 0, 0))
    shape = (lay.rows, lay.half_cols, 3, lay.blocks, LANES)
    return pl.pallas_call(
        functools.partial(sample_kernel, lay),
        grid_spec=pltpu.PrefetchScalarGridSpec(
            num_scalar_prefetch=2,
            grid=(lay.rows, lay.half_cols),
            in_specs=atom_specs(lay) + [field, field],
            out_specs=pl.BlockSpec((1, 1) + shape[2:], lambda row, part, *refs: (row, part, 0, 0, 0)),
        ),
        out_shape=jax.ShapeDtypeStruct(shape, jnp.float32),
        compiler_params=pltpu.CompilerParams(vmem_limit_bytes=40 * 1024 * 1024),
        cost_estimate=pl.CostEstimate(flops=10**10, bytes_accessed=10**7, transcendentals=0),
        name="sample",
    )(starts, turns, atoms, *waves, high, low)


def transform_kernel(
    lay,
    mesh_ref,
    *refs,
):
    message_refs = refs[: lay.rows]
    (
        first_high,
        first_low,
        second_high,
        second_low,
        back_high,
        back_low,
        last_high,
        last_low,
        out_high,
        out_low,
        field_ref,
        mine_ref,
        send_ref,
        recv_ref,
        home_ref,
        extra_ref,
        green_ref,
        send_sem,
        recv_sem,
        back_sem,
        home_sem,
        green_sem,
        high_ref,
        low_ref,
        out_sem,
    ) = refs[lay.rows :]
    row = lax.axis_index("row")
    col = lax.axis_index("col")
    side = col % 2
    partner = (row, col + 1 - 2 * side)
    lines, length, own, padded = lay.lines, lay.length, lay.own, lay.slots_padded
    inner = lines - HALO

    number = message_number(lay, row, col)

    def green_copy(index):
        spot = lax.rem(index - number + lay.rows, lay.rows)
        return pltpu.make_async_copy(message_refs[index], green_ref.at[spot], green_sem.at[index])

    for index in range(lay.rows):
        green_copy(index).start()

    def three(high, low, table_high, table_low):
        return dot(high, table_high) + dot(low, table_high) + dot(high, table_low)

    def push(index):
        return pltpu.make_async_remote_copy(
            src_ref=send_ref.at[index],
            dst_ref=recv_ref.at[index],
            send_sem=send_sem.at[index],
            recv_sem=recv_sem.at[index],
            device_id=partner,
            device_id_type=MESH,
        )

    def push_back(index):
        return pltpu.make_async_remote_copy(
            src_ref=send_ref.at[index],
            dst_ref=home_ref.at[index],
            send_sem=back_sem.at[index],
            recv_sem=home_sem.at[index],
            device_id=partner,
            device_id_type=MESH,
        )

    def forward(slot):
        rows = [
            jnp.concatenate(
                [mesh_ref[r, pl.ds(start, lines, stride=lay.stride), :] for r in range(lay.rows)],
                axis=1,
            )
            for start in (slot, padded + slot)
        ]
        high, low = halves_of(jnp.concatenate(rows, axis=0))
        found = three(high, low, first_high[...], first_low[...])
        upper, lower = found[:lines], found[lines:]
        return upper[:, :length], upper[:, length:], lower[:, :length], lower[:, length:]

    for base, target in ((0, send_ref), (own, mine_ref)):
        away = base == 0

        @pl.loop(0, own)
        def first_pass(i):
            real_cos, real_sin, imag_cos, imag_sin = forward(base + i)

            @pl.when(i == 0)
            def mirrored():
                target[own, 0] = real_cos - imag_sin
                target[own, 1] = -imag_cos - real_sin

            target[i, 0] = real_cos + imag_sin
            target[i, 1] = imag_cos - real_sin
            if away:

                @pl.when(i == 0)
                def start_mirrored():
                    push(own).start()

                push(i).start()

    @pl.loop(0, own + 1)
    def sent(i):
        push(i).wait_send()

    for index in range(lay.rows):
        green_copy(index).wait()

    def spectrum(index):
        mine, other = mine_ref[index], recv_ref[index]
        parts = []
        for part in range(2):
            a, b = mine[part], other[part]
            parts.append(
                jnp.concatenate(
                    [
                        a[HALO:inner],
                        a[inner:] + b[:HALO],
                        b[HALO:inner],
                        b[inner:] + a[:HALO],
                    ],
                    axis=0,
                )
            )
        high, low = halves_of(jnp.concatenate(parts, axis=1))
        found = (
            dot(second_high[...], high) + dot(second_high[...], low) + dot(second_low[...], high)
        )
        cos_part, sin_part = found[:length], found[length:]
        real = cos_part[:, :length] + sin_part[:, length:]
        imag = cos_part[:, length:] - sin_part[:, :length]
        blocks = [green_ref[r, index] for r in range(lay.rows)]
        green = jnp.concatenate(blocks, axis=0)
        return real * green, imag * green

    push(own).wait_recv()
    extra_ref[0], extra_ref[1] = spectrum(own)

    @pl.loop(0, own)
    def second_pass(i):
        push(i).wait_recv()
        real, imag = spectrum(i)
        first = jnp.where(i == 0, 1.0, 0.0)
        real += first * extra_ref[0]
        imag += first * extra_ref[1]
        high, low = halves_of(jnp.concatenate([real, imag], axis=1))
        found = dot(back_high[...], high) + dot(back_high[...], low) + dot(back_low[...], high)
        cos_part, sin_part = found[: 2 * lines], found[2 * lines :]
        real = cos_part[:, :length] - sin_part[:, length:]
        imag = cos_part[:, length:] + sin_part[:, :length]
        mine_ref[i, 0] = real[:lines]
        mine_ref[i, 1] = imag[:lines]
        send_ref[i, 0] = real[lines:]
        send_ref[i, 1] = imag[lines:]
        push_back(i).start()

    cleared = 0 if lay.slots < padded else lines * lay.stride // 8 * 8
    total_rows = mesh_ref.shape[1]
    for r in range(lay.rows):
        field_ref[r, pl.ds(cleared, total_rows - cleared), :] = jnp.zeros(
            (total_rows - cleared, LANES), jnp.float32
        )

    def last(local, planes_ref, i):
        high, low = halves_of(jnp.concatenate([planes_ref[i, 0], planes_ref[i, 1]], axis=0))
        found = three(high, low, last_high[...], last_low[...])
        width = lay.rows * LANES
        real = found[:lines, :width] - found[lines:, width:]
        imag = found[:lines, width:] + found[lines:, :width]
        for part, value in enumerate((real, imag)):
            where = pl.ds(part * padded + local, lines, stride=lay.stride)
            for r in range(lay.rows):
                field_ref[r, where, :] = value[:, r * LANES : (r + 1) * LANES]

    @pl.loop(0, own)
    def last_mine(i):
        last(own + i, mine_ref, i)

    @pl.loop(0, own)
    def last_home(i):
        push_back(i).wait_recv()
        last(i, home_ref, i)

    def leave(r):
        return (
            pltpu.make_async_copy(high_ref.at[r], out_high.at[r], out_sem.at[0, r]),
            pltpu.make_async_copy(low_ref.at[r], out_low.at[r], out_sem.at[1, r]),
        )

    for r in range(lay.rows):

        @pl.loop(0, lay.lines_padded, step=8)
        def split(base):
            for line in range(8):
                first = pl.multiple_of((base + line) * lay.wave_rows, lay.wave_rows)
                where = pl.ds(first, lay.wave_rows)
                value = field_ref[r, pl.ds((base + line) * lay.stride, lay.wave_rows), :]
                high_ref[r, where, :], low_ref[r, where, :] = halves_of(value)

        for copy in leave(r):
            copy.start()

    @pl.loop(0, own)
    def returned(i):
        push_back(i).wait_send()

    for r in range(lay.rows):
        for copy in leave(r):
            copy.wait()


def message_number(lay, row, col):
    member = lax.rem(row, lay.group)
    frame = row // lay.group
    return (lax.rem(col, 2) * lay.frames + frame) * lay.splits + lax.rem(member, lay.splits)


def transform(lay, mesh, messages, tables):
    dma = pltpu.SemaphoreType.DMA
    plane = (2, lay.lines, lay.length)
    vmem = pl.BlockSpec(memory_space=pltpu.VMEM)
    out = jax.ShapeDtypeStruct(
        (lay.rows, lay.lines_padded * lay.wave_rows, LANES), jnp.bfloat16
    )
    return pl.pallas_call(
        functools.partial(transform_kernel, lay),
        in_specs=[vmem] + [pl.BlockSpec(memory_space=pl.ANY)] * lay.rows + [vmem] * len(tables),
        out_specs=[pl.BlockSpec(memory_space=pltpu.HBM)] * 2,
        out_shape=[out, out],
        scratch_shapes=[
            pltpu.VMEM(mesh.shape, jnp.float32),
            pltpu.VMEM((lay.own + 1,) + plane, jnp.float32),
            pltpu.VMEM((lay.own + 1,) + plane, jnp.float32),
            pltpu.VMEM((lay.own + 1,) + plane, jnp.float32),
            pltpu.VMEM((lay.own,) + plane, jnp.float32),
            pltpu.VMEM((2, lay.length, lay.length), jnp.float32),
            pltpu.VMEM((lay.rows,) + messages[0].shape, jnp.float32),
            dma((lay.own + 1,)),
            dma((lay.own + 1,)),
            dma((lay.own,)),
            dma((lay.own,)),
            dma((lay.rows,)),
            pltpu.VMEM(out.shape, jnp.bfloat16),
            pltpu.VMEM(out.shape, jnp.bfloat16),
            dma((2, lay.rows)),
        ],
        compiler_params=pltpu.CompilerParams(
            has_side_effects=True, vmem_limit_bytes=62 * 1024 * 1024
        ),
        cost_estimate=pl.CostEstimate(flops=10**10, bytes_accessed=10**7, transcendentals=0),
        name="transform",
    )(mesh, *messages, *tables)


def table_halves(value):
    leading = lax.reduce_precision(value, exponent_bits=8, mantissa_bits=7)
    return leading.astype(jnp.bfloat16), (value - leading).astype(jnp.bfloat16)


def constant_halves(value):
    high = value.astype(jnp.bfloat16)
    return high, (value - high.astype(np.float64)).astype(jnp.bfloat16)


def make_tables(lay):
    length, half = lay.length, lay.half_cols * lay.block_cols
    waves = np.arange(length)
    spots = np.arange(LANES)
    across = (np.arange(lay.rows)[:, None] * lay.block_rows + spots[None, :] - HALO).reshape(-1)
    valid = np.tile(spots < lay.span, lay.rows)
    angle = across[:, None] * waves[None, :] % length * (2.0 * np.pi / length)
    cosine = np.where(valid[:, None], np.cos(angle), 0.0)
    sine = np.where(valid[:, None], np.sin(angle), 0.0)
    first = constant_halves(np.concatenate([cosine, sine], axis=1))
    last = constant_halves(np.concatenate([cosine.T, sine.T], axis=1))
    zero = lax.optimization_barrier(jnp.int32(0))
    waves = jnp.arange(length, dtype=jnp.int32)
    second = jnp.concatenate(phases(waves[:, None] * (waves[None, :] + zero), length), axis=0)
    near = jnp.arange(lay.lines, dtype=jnp.int32) - HALO + length + zero
    both = jnp.concatenate([near, near + half])
    back = jnp.concatenate(phases(both[:, None] * waves[None, :], length), axis=0)
    tables = []
    for pair in (first, table_halves(second), table_halves(back), last):
        tables.extend(pair)
    return tables


def make_waves(lay, row, col, side):
    length = lay.length
    member = row % lay.group
    source = 2 * (col // 2) + member // lay.splits
    split = member % lay.splits
    start = lay.block_cols * source + jnp.where(source >= lay.half_cols, 1, 0) + split * lay.slots
    index = jnp.arange(lay.slots_padded, dtype=jnp.int32)
    slot = jnp.where(index < lay.own, (1 - side) * lay.own, side * lay.own) + index % lay.own
    waves = start + slot
    packed = (source == 0) & (split == 0) & (slot == 0) & (index < lay.slots)
    live = (index < lay.slots)[None, :, None]
    offsets = jnp.arange(6, dtype=jnp.int32)
    cosine, sine = phases(offsets[:, None] * waves[None, :], length)
    shape = (lay.slots_padded, LANES)
    cosines = jnp.broadcast_to(jnp.where(live, cosine[:, :, None], 0.0), (6,) + shape)
    sines = jnp.broadcast_to(jnp.where(live, sine[:, :, None], 0.0), (6,) + shape)
    return (
        jnp.broadcast_to(waves[:, None], shape),
        jnp.broadcast_to(packed[:, None].astype(jnp.float32), shape),
        cosines,
        sines,
    )


def share_green(lay, influence, row, col):
    length = lay.length
    rows, cols = lay.rows, lay.cols
    scale = 1.0 / float(length) ** 3
    used = lay.block_cols // 2
    offset = jnp.where(col >= lay.half_cols, 1, 0)
    middle = lax.ppermute(influence[:, 0, :], "col", [(lay.half_cols, 0)])
    block = lax.dynamic_slice_in_dim(influence, offset, used, axis=1).transpose(1, 0, 2)
    block = block.reshape(lay.splits, 2, lay.own, lay.block_rows, length)
    special = col == 0
    zeroth = block[0, 0, 0]
    extra = jnp.where(special, (0.5 * scale) * (zeroth - middle), 0.0)
    zeroth = jnp.where(special, (0.5 * scale) * (zeroth + middle), (2.0 * scale) * zeroth)
    block = jnp.concatenate([(2.0 * scale) * block, jnp.zeros_like(block[:, :, :1])], axis=2)
    block = block.at[0, 0, 0].set(zeroth).at[0, 0, lay.own].set(extra)
    block = block.reshape((2 * lay.splits,) + block.shape[2:])
    messages = []
    for number in range(rows):
        message = (number - row) % rows
        split = message % lay.splits
        side = message // (lay.frames * lay.splits)
        sent = lax.dynamic_index_in_dim(block, split * 2 + side, keepdims=False)
        pairs = []
        for r in range(rows):
            at = (number - r) % rows
            to_split, rest = at % lay.splits, at // lay.splits
            to_frame, to_side = rest % lay.frames, rest // lay.frames
            for c in range(cols):
                to_row = to_frame * lay.group + (c % 2) * lay.splits + to_split
                pairs.append((r * cols + c, to_row * cols + 2 * (c // 2) + to_side))
        messages.append(lax.ppermute(sent, ("row", "col"), pairs))
    return messages


def forces_of(cell_index, fraction, charge, atom_count, influence):
    frames, _, atoms = fraction.shape
    lay = Layout(frames, influence.shape[2], atoms)
    row = lax.axis_index("row")
    col = lax.axis_index("col")
    side = col % 2
    messages = share_green(lay, influence, row, col)
    tables = make_tables(lay)
    waves = make_waves(lay, row, col, side)

    slot_ids = jnp.arange(atoms, dtype=jnp.int32)
    alive = slot_ids[None, :] < atom_count
    charges = jnp.where(alive, charge, 0.0)
    origin = jnp.stack([row * lay.block_rows, (col // lay.half_cols) * lay.half_cols * lay.block_cols, 0])
    cells = cell_index - origin[None, :, None]
    payload = jnp.concatenate(
        [
            cells.astype(jnp.float32),
            fraction,
            charges[:, None, :],
            alive[:, None, :].astype(jnp.float32),
        ],
        axis=1,
    )
    sorted_atoms, rank = sort_atoms(lay, payload)
    shared = gather_atoms(lay, sorted_atoms)

    lines = shared[:, :, 1, :].reshape(lay.rows * lay.half_cols * lay.blocks, LANES)
    lives = shared[:, :, 7, :].reshape(lines.shape) > 0.5
    lowest = jnp.min(jnp.where(lives, lines, 1024.0), axis=1).astype(jnp.int32)
    highest = jnp.max(jnp.where(lives, lines, -1024.0), axis=1).astype(jnp.int32)
    live = highest >= lowest
    starts = jnp.where(live, lowest + HALO - 5, 0)
    turns = jnp.where(live, (highest - lowest + 6 + CHUNK - 1) // CHUNK, 0)

    mesh = spread(lay, starts, turns, shared, waves)
    high, low = transform(lay, mesh, messages, tables)
    partial = sample(lay, starts, turns, shared, waves, high, low)
    returned = return_forces(lay, partial)
    forces = jnp.sum(returned, axis=1).reshape(frames, 3, atoms)
    forces = jnp.pad(forces, ((0, 0), (0, 5), (0, 0)))
    return unsort_forces(rank, forces)[:, :3]


def solution(mesh):
    placed = (
        P(None, None, ("row", "col")),
        P(None, None, ("row", "col")),
        P(None, ("row", "col")),
        P(None, ("row", "col")),
        P("row", "col", None),
    )
    return jax.shard_map(
        forces_of, mesh=mesh, in_specs=placed, out_specs=P(None, None, ("row", "col")), check_vma=False
    )
```
